32 devices in a mesh: seq: 16 (over z, y, x), head: 2 (over core).
Axes of the slice: x: 2, y: 2, z: 4, core: 2. Of those that a mesh axis runs over, the one named last changes fastest.
Arguments:
- query_rows: bfloat16 [16, 4096, 128], P('head', 'seq'), may hold values from -6 to 6
- key_rows: bfloat16 [16, 4096, 128], P('head', 'seq'), may hold values from -6 to 6
- value_rows: bfloat16 [16, 4096, 128], P('head', 'seq'), may hold values from -6 to 6
- norm_gain: float32 [16, 128], P('head'), may hold values from 0.25 to 1.75
- level_table: float32 [16, 16, 6], P(None, 'head'), may hold values from 0.3 to 4.5
- level_index: int32 [4096, 6], P('seq'), may hold values from 0 to 15
- window_length: int32 [16], P('head'), may hold values from 512 to 1024, as said below
- out_grad: bfloat16 [16, 4096, 128], P('head', 'seq'), may hold values from -18 to 18
Outputs:
- layer_out: bfloat16 [16, 4096, 128], P('head', 'seq')
- query_grad: bfloat16 [16, 4096, 128], P('head', 'seq')
- key_grad: bfloat16 [16, 4096, 128], P('head', 'seq')
- value_grad: bfloat16 [16, 4096, 128], P('head', 'seq')
- table_grad: float32 [16, 16, 6], P(None, 'head')
- gain_grad: float32 [16, 128], P('head')
The draws below stay inside these ranges and needn't reach their ends.
Inputs may be any that keep to these rules, and one draw needn't show every extreme that they name: `window_length`: every head's window holds at least half of 1024 tokens and at most 1024; some head's window is exactly 1024.
All inputs are finite; a program needn't handle non-finite values.
Results may differ from the reference program's by a relative error of at most 0.0078.
Values may be sent and summed in bfloat16 or wider, within the bound.
No kernel may reach another device: no remote copies, remote signals or barrier semaphores. Data moves between devices by JAX's collectives and lax.ppermute only.
A program may use at most 128 MiB of HBM per device.

```python
import math
import jax
import jax.numpy as jnp
from jax import lax

H = 16
HD = 128
BLOCK = 64
WINDOW = 1024
LEVELS = 6
TABLE_ROWS = 16
TOKENS = 4096


def draw_level_table(key, part):
    ramp = 1.0 + 2.0 * jnp.arange(H, dtype=jnp.float32) / (H - 1)
    base = jnp.exp(jax.random.uniform(key, (TABLE_ROWS, H, LEVELS), jnp.float32, math.log(0.3), math.log(1.5)))
    return base * ramp[None, :, None]


def draw_window_length(key, part):
    lengths = jax.random.randint(jax.random.fold_in(key, 11), (H,), WINDOW // 2, WINDOW + 1, dtype=jnp.int32)
    chosen = jax.random.randint(jax.random.fold_in(key, 12), (), 0, H, dtype=jnp.int32)
    return jnp.where(jnp.arange(H, dtype=jnp.int32) == chosen, WINDOW, lengths).astype(jnp.int32)


def draw_out_grad(key, part):
    ramp = 1.0 + 2.0 * jnp.arange(TOKENS, dtype=jnp.float32) / (TOKENS - 1)
    base = jnp.clip(jax.random.normal(key, (H, TOKENS, HD), jnp.float32), -6.0, 6.0)
    return (base * ramp[None, :, None]).astype(jnp.bfloat16)


def place_ends(result, rng, smallest, high):
    index_at = [jax.random.randint(jax.random.fold_in(rng, axis), (), 0, length) for axis, length in enumerate(result.shape)]
    main_axis = result.shape.index(max(result.shape))
    beside = index_at[:main_axis] + [(index_at[main_axis] + 1) % result.shape[main_axis]] + index_at[main_axis + 1:]
    return result.at[tuple(index_at)].set(smallest).at[tuple(beside)].set(high)


def levels(key, dims, split, smallest, high):
    gain = 1.0
    for dim, blocks in split:
        steps = jax.random.uniform(jax.random.fold_in(jax.random.fold_in(key, 6), dim), (blocks,), jnp.float32, smallest / len(split), high / len(split))
        gain = gain * jnp.repeat(jnp.exp(steps), dims[dim] // blocks).reshape((-1,) + (1,) * (len(dims) - 1 - dim))
    return gain


def bell_draw(rng, extent, deviation, limit, cuts=(), kind=jnp.bfloat16):
    entries = jax.random.normal(rng, extent, jnp.float32) * deviation
    if len(cuts) > 0:
        entries = levels(rng, extent, cuts, -0.22, 0.18) * entries
    return jnp.clip(entries, min=-limit, max=limit).astype(kind)


def setup_inputs(seed: int = 0) -> dict:
    streams_of = jax.random.split(jax.random.key(seed), 9)
    query_rows = bell_draw(streams_of[0], (H, TOKENS, HD), 1.0, 6.0, ((0, 2), (1, 16)))
    key_rows = bell_draw(streams_of[1], (H, TOKENS, HD), 1.0, 6.0, ((0, 2), (1, 16)))
    value_rows = bell_draw(streams_of[2], (H, TOKENS, HD), 1.0, 6.0, ((0, 2), (1, 16)))
    norm_gain = jnp.clip(1.0 + 0.15 * jax.random.normal(streams_of[3], (H, HD), jnp.float32), 0.25, 1.75)
    level_table = draw_level_table(jax.random.fold_in(streams_of[8], 71), 0)
    level_index = place_ends(jax.random.randint(streams_of[5], (TOKENS, LEVELS), 0, TABLE_ROWS), jax.random.fold_in(streams_of[5], 1), 0, TABLE_ROWS - 1).astype(jnp.int32)
    window_length = draw_window_length(jax.random.fold_in(streams_of[8], 71), 0)
    out_grad = draw_out_grad(jax.random.fold_in(streams_of[8], 71), 0)
    return {"query_rows": query_rows, "key_rows": key_rows, "value_rows": value_rows, "norm_gain": norm_gain, "level_table": level_table, "level_index": level_index, "window_length": window_length, "out_grad": out_grad}


epsilon = 1e-06
block_cap = 512

def product(pattern, left_side, right_side):
    return jnp.einsum(pattern, left_side.astype(jnp.float32), right_side.astype(jnp.float32), precision=lax.Precision.HIGHEST)

def causal_mask():
    row_pos = lax.broadcasted_iota(jnp.int32, (BLOCK, BLOCK), 0)
    col_pos = lax.broadcasted_iota(jnp.int32, (BLOCK, BLOCK), 1)
    return row_pos >= col_pos

def window_mask(block_rows, span_len):
    query_pos = lax.broadcasted_iota(jnp.int32, (1, block_rows, WINDOW + block_rows), 1)
    key_pos = lax.broadcasted_iota(jnp.int32, (1, block_rows, WINDOW + block_rows), 2)
    offset = query_pos + WINDOW - key_pos
    return (offset >= 0) & (offset < span_len[:, None, None])

def leaf_view(tensor):
    head_count, token_count, head_dim = tensor.shape
    return tensor.reshape(head_count, token_count // BLOCK, BLOCK, head_dim)

def split_level(tensor, group_len):
    head_count, token_count, head_dim = tensor.shape
    return tensor.reshape(head_count, token_count // (2 * group_len), 2, group_len, head_dim)

def level_summary(key_rows, value_rows, group_len):
    lower_sum = product('hpse,hpsf->hpef', split_level(key_rows, group_len)[:, :, 0], split_level(value_rows, group_len)[:, :, 0])
    return (lower_sum * (1.0 / math.sqrt(group_len * key_rows.shape[-1]))).astype(jnp.bfloat16)

def level_area(query_rows, summary, group_len):
    upper_half = product('hpse,hpef->hpsf', split_level(query_rows, group_len)[:, :, 1], summary)
    return jnp.stack([jnp.zeros_like(upper_half), upper_half], axis=2).reshape(query_rows.shape)

def level_grads(query_rows, key_rows, value_rows, summary, upstream, group_len):
    upstream_up = split_level(upstream, group_len)[:, :, 1]
    query_up = product('hpsf,hpef->hpse', upstream_up, summary)
    summary_grad = product('hpse,hpsf->hpef', split_level(query_rows, group_len)[:, :, 1], upstream_up)
    low_grad = (summary_grad * (1.0 / math.sqrt(group_len * query_rows.shape[-1]))).astype(jnp.bfloat16)
    key_low = product('hpsf,hpef->hpse', split_level(value_rows, group_len)[:, :, 0], low_grad)
    value_low = product('hpse,hpef->hpsf', split_level(key_rows, group_len)[:, :, 0], low_grad)
    blank = jnp.zeros_like(query_up)
    full_shape = query_rows.shape
    return (jnp.stack([blank, query_up], axis=2).reshape(full_shape), jnp.stack([key_low, blank], axis=2).reshape(full_shape), jnp.stack([value_low, blank], axis=2).reshape(full_shape))

def window_setup(query_rows, key_rows, value_rows, window_length):
    head_count, token_count, head_dim = query_rows.shape
    block_rows = min(block_cap, token_count)
    padding = jnp.zeros((head_count, WINDOW, head_dim), jnp.bfloat16)
    key_pad = jnp.concatenate([padding, key_rows], axis=1)
    value_pad = jnp.concatenate([padding, value_rows], axis=1)
    score_scale = lax.rsqrt((head_dim * window_length).astype(jnp.float32))[:, None, None]
    inside = window_mask(block_rows, window_length)
    return (block_rows, key_pad, value_pad, score_scale, inside)

def window_forward(query_rows, key_rows, value_rows, window_length):
    token_count = query_rows.shape[1]
    block_rows, key_pad, value_pad, score_scale, inside = window_setup(query_rows, key_rows, value_rows, window_length)

    def one_block(block_no):
        row_start = block_no * block_rows
        query_part = lax.dynamic_slice_in_dim(query_rows, row_start, block_rows, 1)
        key_part = lax.dynamic_slice_in_dim(key_pad, row_start, WINDOW + block_rows, 1)
        value_part = lax.dynamic_slice_in_dim(value_pad, row_start, WINDOW + block_rows, 1)
        prob_low = jnp.where(inside, product('hqe,hke->hqk', query_part, key_part) * score_scale, 0.0).astype(jnp.bfloat16)
        return product('hqk,hke->hqe', prob_low, value_part)
    blocks = lax.map(one_block, jnp.arange(token_count // block_rows, dtype=jnp.int32))
    return jnp.transpose(blocks, (1, 0, 2, 3)).reshape(query_rows.shape)

def window_backward(query_rows, key_rows, value_rows, grad_low, window_length):
    head_count, token_count, head_dim = query_rows.shape
    block_rows, key_pad, value_pad, score_scale, inside = window_setup(query_rows, key_rows, value_rows, window_length)

    def one_block(pending, block_no):
        key_acc, value_acc = pending
        row_start = block_no * block_rows
        query_part = lax.dynamic_slice_in_dim(query_rows, row_start, block_rows, 1)
        grad_part = lax.dynamic_slice_in_dim(grad_low, row_start, block_rows, 1)
        key_part = lax.dynamic_slice_in_dim(key_pad, row_start, WINDOW + block_rows, 1)
        value_part = lax.dynamic_slice_in_dim(value_pad, row_start, WINDOW + block_rows, 1)
        prob_low = jnp.where(inside, product('hqe,hke->hqk', query_part, key_part) * score_scale, 0.0).astype(jnp.bfloat16)
        prob_grad = product('hqe,hke->hqk', grad_part, value_part)
        score_grad = jnp.where(inside, prob_grad * score_scale, 0.0).astype(jnp.bfloat16)
        query_part_grad = product('hqk,hke->hqe', score_grad, key_part)
        key_new = lax.dynamic_slice_in_dim(key_acc, row_start, WINDOW + block_rows, 1) + product('hqk,hqe->hke', score_grad, query_part)
        value_new = lax.dynamic_slice_in_dim(value_acc, row_start, WINDOW + block_rows, 1) + product('hqk,hqe->hke', prob_low, grad_part)
        anchor = jnp.zeros((), jnp.int32)
        key_acc = lax.dynamic_update_slice(key_acc, key_new, (anchor, row_start, anchor))
        value_acc = lax.dynamic_update_slice(value_acc, value_new, (anchor, row_start, anchor))
        return ((key_acc, value_acc), query_part_grad)
    start_acc = jnp.zeros((head_count, WINDOW + token_count, head_dim), jnp.float32)
    (key_acc, value_acc), blocks = lax.scan(one_block, (start_acc, start_acc), jnp.arange(token_count // block_rows, dtype=jnp.int32))
    query_grad = jnp.transpose(blocks, (1, 0, 2, 3)).reshape(query_rows.shape)
    return (query_grad, key_acc[:, WINDOW:], value_acc[:, WINDOW:])

def reference(query_rows, key_rows, value_rows, norm_gain, level_table, level_index, window_length, out_grad):
    head_count, token_count, head_dim = query_rows.shape
    top_level = (token_count // BLOCK).bit_length() - 1
    onehot = (level_index[:, :, None] == jnp.arange(TABLE_ROWS, dtype=jnp.int32)[None, None, :]).astype(jnp.float32)
    weights = jnp.einsum('tjk,khj->htj', onehot, level_table, precision=lax.Precision.HIGHEST)

    def weight_of(level_no):
        return weights[:, :, min(level_no, LEVELS - 1)][:, :, None]
    query_leaf = leaf_view(query_rows)
    key_leaf = leaf_view(key_rows)
    value_leaf = leaf_view(value_rows)
    leaf_scale = 1.0 / math.sqrt(BLOCK * head_dim)
    causal = causal_mask()
    leaf_prob = jnp.where(causal, product('hcte,hcse->hcts', query_leaf, key_leaf) * leaf_scale, 0.0).astype(jnp.bfloat16)
    leaf_area = product('hcts,hcse->hcte', leaf_prob, value_leaf).reshape(query_rows.shape)
    mixed = window_forward(query_rows, key_rows, value_rows, window_length) + weight_of(0) * leaf_area
    for level_no in range(1, top_level + 1):
        group_len = BLOCK * 2 ** (level_no - 1)
        summary = level_summary(key_rows, value_rows, group_len)
        mixed = mixed + weight_of(level_no) * level_area(query_rows, summary, group_len)
    inv_rms = lax.rsqrt(lax.optimization_barrier(jnp.sum(mixed * mixed, axis=(0, 2))) / (head_count * head_dim) + epsilon)
    layer_out = (mixed * inv_rms[None, :, None] * norm_gain[:, None, :]).astype(jnp.bfloat16)
    grad_full = out_grad.astype(jnp.float32)
    scaled = grad_full * norm_gain[:, None, :]
    cross_sum = lax.optimization_barrier(jnp.sum(scaled * mixed, axis=(0, 2)))
    mixed_grad = scaled * inv_rms[None, :, None] - mixed * (inv_rms ** 3 * cross_sum / (head_count * head_dim))[None, :, None]
    gain_grad = lax.optimization_barrier(jnp.sum(grad_full * mixed * inv_rms[None, :, None], axis=1))
    grad_low = mixed_grad.astype(jnp.bfloat16)
    columns = [jnp.zeros((head_count, token_count), jnp.float32) for column_no in range(LEVELS)]
    columns[0] = columns[0] + lax.optimization_barrier(jnp.sum(mixed_grad * leaf_area, axis=2))
    upstream_leaf = leaf_view((weight_of(0) * mixed_grad).astype(jnp.bfloat16))
    prob_grad = product('hcte,hcse->hcts', upstream_leaf, value_leaf)
    score_grad = jnp.where(causal, prob_grad * leaf_scale, 0.0).astype(jnp.bfloat16)
    query_grad = product('hcts,hcse->hcte', score_grad, key_leaf).reshape(query_rows.shape)
    key_grad = product('hcts,hcte->hcse', score_grad, query_leaf).reshape(query_rows.shape)
    value_grad = product('hcts,hcte->hcse', leaf_prob, upstream_leaf).reshape(query_rows.shape)
    window_query, window_key, window_value = window_backward(query_rows, key_rows, value_rows, grad_low, window_length)
    query_grad = query_grad + window_query
    key_grad = key_grad + window_key
    value_grad = value_grad + window_value
    for level_no in range(1, top_level + 1):
        group_len = BLOCK * 2 ** (level_no - 1)
        summary = level_summary(key_rows, value_rows, group_len)
        area_now = level_area(query_rows, summary, group_len)
        column_no = min(level_no, LEVELS - 1)
        columns[column_no] = columns[column_no] + lax.optimization_barrier(jnp.sum(mixed_grad * area_now, axis=2))
        upstream = (weight_of(level_no) * mixed_grad).astype(jnp.bfloat16)
        query_part, key_part, value_part = level_grads(query_rows, key_rows, value_rows, summary, upstream, group_len)
        query_grad = query_grad + query_part
        key_grad = key_grad + key_part
        value_grad = value_grad + value_part
    weight_grad = jnp.stack(columns, axis=-1)
    table_grad = jnp.einsum('tjk,htj->khj', onehot, weight_grad, precision=lax.Precision.HIGHEST)
    return (layer_out, query_grad.astype(jnp.bfloat16), key_grad.astype(jnp.bfloat16), value_grad.astype(jnp.bfloat16), table_grad, gain_grad)
```

```python
import functools
import math

import jax
import jax.numpy as jnp
from jax import lax
from jax.experimental import pallas as pl
from jax.experimental.pallas import tpu as pltpu
from jax.sharding import PartitionSpec as P

H = 16
BLOCK = 64
WINDOW = 1024
LEVELS = 6
TABLE_ROWS = 16


epsilon = 1e-06
block_cap = 512


def shifted(block, axis, distance):
    devices = range(lax.axis_size(axis))
    route = [(i - distance, i) for i in devices if i - distance in devices]
    return lax.ppermute(block, axis, route)


def from_partner(shard, axis, bit):
    return lax.ppermute(shard, axis, [(i, i ^ 1 << bit) for i in range(lax.axis_size(axis))])


def contract(pattern, left_side, right_side):
    return jnp.einsum(pattern, left_side, right_side, preferred_element_type=jnp.float32)


def causal_mask():
    row_pos = lax.broadcasted_iota(jnp.int32, (BLOCK, BLOCK), 0)
    col_pos = lax.broadcasted_iota(jnp.int32, (BLOCK, BLOCK), 1)
    return row_pos >= col_pos


def window_mask(block_rows, shift_rows, key_count, span_len):
    query_pos = lax.broadcasted_iota(jnp.int32, (block_rows, key_count), 0)
    key_pos = lax.broadcasted_iota(jnp.int32, (block_rows, key_count), 1)
    offset = query_pos + shift_rows - key_pos
    return (offset >= 0) & (offset < span_len)


def leaf_view(tensor):
    head_count, token_count, head_dim = tensor.shape
    return tensor.reshape(head_count, token_count // BLOCK, BLOCK, head_dim)


def split_level(tensor, group_len):
    head_count, token_count, head_dim = tensor.shape
    return tensor.reshape(head_count, token_count // (2 * group_len), 2, group_len, head_dim)


def level_summary(key_rows, value_rows, group_len):
    lower_sum = contract(
        "hpse,hpsf->hpef",
        split_level(key_rows, group_len)[:, :, 0],
        split_level(value_rows, group_len)[:, :, 0],
    )
    return (lower_sum * (1.0 / math.sqrt(group_len * key_rows.shape[-1]))).astype(jnp.bfloat16)


def level_area(query_rows, summary, group_len):
    upper_half = contract("hpse,hpef->hpsf", split_level(query_rows, group_len)[:, :, 1], summary)
    return jnp.stack([jnp.zeros_like(upper_half), upper_half], axis=2).reshape(query_rows.shape)


def level_grads(query_rows, key_rows, value_rows, summary, upstream, group_len):
    upstream_up = split_level(upstream, group_len)[:, :, 1]
    query_up = contract("hpsf,hpef->hpse", upstream_up, summary)
    summary_grad = contract(
        "hpse,hpsf->hpef", split_level(query_rows, group_len)[:, :, 1], upstream_up
    )
    low_grad = (summary_grad * (1.0 / math.sqrt(group_len * query_rows.shape[-1]))).astype(
        jnp.bfloat16
    )
    key_low = contract("hpsf,hpef->hpse", split_level(value_rows, group_len)[:, :, 0], low_grad)
    value_low = contract("hpse,hpef->hpsf", split_level(key_rows, group_len)[:, :, 0], low_grad)
    blank = jnp.zeros_like(query_up)
    full_shape = query_rows.shape
    return (
        jnp.stack([blank, query_up], axis=2).reshape(full_shape),
        jnp.stack([key_low, blank], axis=2).reshape(full_shape),
        jnp.stack([value_low, blank], axis=2).reshape(full_shape),
    )


def window_head(query_head, key_head, value_head, span_len):
    token_count, head_dim = query_head.shape
    block_rows = min(block_cap, token_count)
    score_scale = lax.rsqrt((head_dim * span_len).astype(jnp.float32))
    inside = window_mask(block_rows, WINDOW, WINDOW + block_rows, span_len)
    scores = contract("qe,ke->qk", query_head, key_head) * score_scale
    prob_low = jnp.where(inside, scores, 0.0).astype(jnp.bfloat16)
    outputs = [contract("qk,ke->qe", prob_low, value_head)]
    return jnp.concatenate(outputs, axis=0)


def window_back_head(query_head, key_head, value_head, grad_head, span_len, keep_from):
    token_count, head_dim = query_head.shape
    block_rows = min(block_cap, token_count)
    score_scale = lax.rsqrt((head_dim * span_len).astype(jnp.float32))
    inside = window_mask(block_rows, WINDOW, WINDOW + block_rows, span_len)
    key_grad = jnp.zeros((WINDOW + token_count - keep_from, head_dim), jnp.float32)
    value_grad = jnp.zeros((WINDOW + token_count - keep_from, head_dim), jnp.float32)
    grad_part = grad_head[0:block_rows]
    scores = contract("qe,ke->qk", query_head, key_head) * score_scale
    prob_low = jnp.where(inside, scores, 0.0).astype(jnp.bfloat16)
    prob_grad = contract("qe,ke->qk", grad_part, value_head)
    score_grad = jnp.where(inside, prob_grad * score_scale, 0.0).astype(jnp.bfloat16)
    query_grad = [contract("qk,ke->qe", score_grad, key_head)]
    skip_cols = max(keep_from, 0)
    target = skip_cols - keep_from
    length_now = WINDOW + block_rows - skip_cols
    key_grad = key_grad.at[target : target + length_now].add(
        contract("qk,qe->ke", score_grad[:, skip_cols:], query_head)
    )
    value_grad = value_grad.at[target : target + length_now].add(
        contract("qk,qe->ke", prob_low, grad_part)
    )
    return (jnp.concatenate(query_grad, axis=0), key_grad, value_grad)


def wide_shards(
    query_rows, key_rows, value_rows, norm_gain, level_table, level_index, window_length, out_grad
):
    heads_here, tok_here, head_dim = query_rows.shape
    seq_index = lax.axis_index("seq")
    seq_levels = lax.axis_size("seq").bit_length() - 1
    local_levels = (tok_here // BLOCK).bit_length() - 1
    reach_count = WINDOW // tok_here
    onehot = (
        level_index[:, :, None] == lax.broadcasted_iota(jnp.int32, (1, 1, TABLE_ROWS), 2)
    ).astype(jnp.float32)
    weights = jnp.einsum("tjk,khj->htj", onehot, level_table, precision=lax.Precision.HIGHEST)

    def weight_of(level_no):
        return weights[:, :, min(level_no, LEVELS - 1)][:, :, None]

    own_pair = jnp.stack([key_rows, value_rows])
    pieces = []
    for step_no in range(reach_count, 0, -1):
        pieces.append(shifted(own_pair, "seq", step_no))
    pieces.append(own_pair)
    wide_pair = jnp.concatenate(pieces, axis=2)
    device_summary = contract("hte,htf->hef", key_rows, value_rows)
    sibling = []
    running = device_summary
    for bit_no in range(seq_levels):
        partner = from_partner(running, "seq", bit_no)
        upper_half = seq_index >> bit_no & 1 == 1
        sibling.append(jnp.where(upper_half, partner, 0.0))
        running = running + partner
    query_leaf = leaf_view(query_rows)
    key_leaf = leaf_view(key_rows)
    value_leaf = leaf_view(value_rows)
    leaf_scale = 1.0 / math.sqrt(BLOCK * head_dim)
    causal = causal_mask()
    leaf_prob = jnp.where(
        causal, contract("hcte,hcse->hcts", query_leaf, key_leaf) * leaf_scale, 0.0
    ).astype(jnp.bfloat16)
    area_list = [contract("hcts,hcse->hcte", leaf_prob, value_leaf).reshape(query_rows.shape)]
    summaries = []
    for level_no in range(1, local_levels + 1):
        group_len = BLOCK * 2 ** (level_no - 1)
        summary = level_summary(key_rows, value_rows, group_len)
        summaries.append(summary)
        area_list.append(level_area(query_rows, summary, group_len))
    for bit_no in range(seq_levels):
        group_len = tok_here * 2**bit_no
        summary = (sibling[bit_no] * (1.0 / math.sqrt(group_len * head_dim))).astype(jnp.bfloat16)
        summaries.append(summary)
        area_list.append(contract("hte,hef->htf", query_rows, summary))
    mixed = lax.map(
        lambda head_items: window_head(head_items[0], head_items[1], head_items[2], head_items[3]),
        (query_rows, wide_pair[0], wide_pair[1], window_length),
    )
    for level_no in range(len(area_list)):
        mixed = mixed + weight_of(level_no) * area_list[level_no]
    grad_full = out_grad.astype(jnp.float32)
    scaled = grad_full * norm_gain[:, None, :]
    square_sum, cross_sum = lax.psum(
        (jnp.sum(mixed * mixed, axis=(0, 2)), jnp.sum(scaled * mixed, axis=(0, 2))), "head"
    )
    inv_rms = lax.rsqrt(square_sum / (H * head_dim) + epsilon)
    layer_out = (mixed * inv_rms[None, :, None] * norm_gain[:, None, :]).astype(jnp.bfloat16)
    mixed_grad = (
        scaled * inv_rms[None, :, None]
        - mixed * (inv_rms**3 * cross_sum / (H * head_dim))[None, :, None]
    )
    gain_part = jnp.sum(grad_full * mixed * inv_rms[None, :, None], axis=1)
    grad_low = mixed_grad.astype(jnp.bfloat16)
    columns = [jnp.zeros((heads_here, tok_here), jnp.float32) for column_no in range(LEVELS)]
    for level_no in range(len(area_list)):
        column_no = min(level_no, LEVELS - 1)
        columns[column_no] = columns[column_no] + jnp.sum(mixed_grad * area_list[level_no], axis=2)
    upstream_leaf = leaf_view((weight_of(0) * mixed_grad).astype(jnp.bfloat16))
    prob_grad = contract("hcte,hcse->hcts", upstream_leaf, value_leaf)
    score_grad = jnp.where(causal, prob_grad * leaf_scale, 0.0).astype(jnp.bfloat16)
    query_grad = contract("hcts,hcse->hcte", score_grad, key_leaf).reshape(query_rows.shape)
    key_grad = contract("hcts,hcte->hcse", score_grad, query_leaf).reshape(query_rows.shape)
    value_grad = contract("hcts,hcte->hcse", leaf_prob, upstream_leaf).reshape(query_rows.shape)
    for level_no in range(1, local_levels + 1):
        group_len = BLOCK * 2 ** (level_no - 1)
        upstream = (weight_of(level_no) * mixed_grad).astype(jnp.bfloat16)
        query_part, key_part, value_part = level_grads(
            query_rows, key_rows, value_rows, summaries[level_no - 1], upstream, group_len
        )
        query_grad = query_grad + query_part
        key_grad = key_grad + key_part
        value_grad = value_grad + value_part
    summary_grads = []
    for bit_no in range(seq_levels):
        level_no = local_levels + 1 + bit_no
        upstream = (weight_of(level_no) * mixed_grad).astype(jnp.bfloat16)
        query_grad = query_grad + contract("htf,hef->hte", upstream, summaries[level_no - 1])
        group_len = tok_here * 2**bit_no
        partial_value = contract("hte,htf->hef", query_rows, upstream) * (
            1.0 / math.sqrt(group_len * head_dim)
        )
        upper_half = seq_index >> bit_no & 1 == 1
        summary_grads.append(jnp.where(upper_half, partial_value, 0.0))
    pending = jnp.stack(summary_grads)
    for bit_no in range(seq_levels):
        partner = from_partner(pending[bit_no:], "seq", bit_no)
        lower_half = seq_index >> bit_no & 1 == 0
        received = jnp.where(lower_half, partner[0], 0.0).astype(jnp.bfloat16)
        key_grad = key_grad + contract("htf,hef->hte", value_rows, received)
        value_grad = value_grad + contract("hte,hef->htf", key_rows, received)
        pending = jnp.concatenate(
            [pending[: bit_no + 1], pending[bit_no + 1 :] + partner[1:]], axis=0
        )
    keep_from = 0
    window_query, window_key, window_value = lax.map(
        lambda head_items: window_back_head(
            head_items[0], head_items[1], head_items[2], head_items[3], head_items[4], keep_from
        ),
        (query_rows, wide_pair[0], wide_pair[1], grad_low, window_length),
    )
    query_grad = query_grad + window_query
    key_grad = key_grad + window_key[:, WINDOW:]
    value_grad = value_grad + window_value[:, WINDOW:]
    for step_no in range(1, reach_count + 1):
        first_row = (reach_count - step_no) * tok_here
        piece = jnp.stack(
            [
                window_key[:, first_row : first_row + tok_here],
                window_value[:, first_row : first_row + tok_here],
            ]
        )
        arrived = shifted(piece.astype(jnp.bfloat16), "seq", -step_no).astype(piece.dtype)
        key_grad = key_grad + arrived[0]
        value_grad = value_grad + arrived[1]
    weight_grad = jnp.stack(columns, axis=-1)
    table_part = jnp.einsum("tjk,htj->khj", onehot, weight_grad, precision=lax.Precision.HIGHEST)
    table_grad, gain_grad = lax.psum((table_part, gain_part), "seq")
    return (
        layer_out,
        query_grad.astype(jnp.bfloat16),
        key_grad.astype(jnp.bfloat16),
        value_grad.astype(jnp.bfloat16),
        table_grad,
        gain_grad,
    )


f32 = jnp.float32
bf16 = jnp.bfloat16
index_rows = 16


def dot_nn(left, right):
    return lax.dot_general(left, right, (((1,), (0,)), ((), ())), preferred_element_type=f32)


def dot_nt(left, right):
    return lax.dot_general(left, right, (((1,), (1,)), ((), ())), preferred_element_type=f32)


def dot_tn(left, right):
    return lax.dot_general(left, right, (((0,), (0,)), ((), ())), preferred_element_type=f32)


def level_scale(level_no, head_dim):
    return 1.0 / math.sqrt(BLOCK * 2 ** max(level_no - 1, 0) * head_dim)


def lane_indices(index_block):
    rows = index_block.astype(f32)
    return jnp.concatenate([rows[:8], rows[8:]], axis=1)


def lane_weights(indices, table_ref):
    weights = jnp.zeros(indices.shape, f32)
    wide = indices.shape[1] // table_ref.shape[-1]
    for row_no in range(TABLE_ROWS):
        row = jnp.concatenate([table_ref[0, row_no]] * wide, axis=1)
        weights = jnp.where(indices == row_no, row, weights)
    return weights


def columns_of(lanes):
    return jnp.transpose(lanes)


def positions(rows):
    row_pos = lax.broadcasted_iota(jnp.int32, (rows, rows), 0)
    col_pos = lax.broadcasted_iota(jnp.int32, (rows, rows), 1)
    return row_pos, col_pos


def leaf_bits(row_pos, col_pos):
    shift = BLOCK.bit_length() - 1
    return (row_pos >> shift) ^ (col_pos >> shift)


def diagonal_factor(query_pos, key_pos, picked, window_scale, near_levels, head_dim):
    apart = leaf_bits(query_pos, key_pos)
    factor = picked(0) * level_scale(0, head_dim)
    for level_no in range(1, near_levels + 1):
        factor = jnp.where(
            apart >= 2 ** (level_no - 1), picked(level_no) * level_scale(level_no, head_dim), factor
        )
    return jnp.where(query_pos >= key_pos, factor + window_scale, 0.0)


def fill(target, first_ref, second_ref):
    count, rows, _ = first_ref.shape
    for block_no in range(count):
        target[pl.ds(block_no * rows, rows)] = first_ref[block_no]
        target[pl.ds((count + block_no) * rows, rows)] = second_ref[block_no]


def summary_kernel(key_ref, value_ref, near_ref, total_ref, *, near_levels):
    group, _, head_dim = key_ref.shape
    parts = [dot_tn(key_ref[block_no], value_ref[block_no]) for block_no in range(group)]
    total_ref[0] = functools.reduce(lambda a, b: a + b, parts)
    for block_no in range(group):
        for bit_no in range(group.bit_length() - 1):
            if block_no >> bit_no & 1:
                first = (block_no >> bit_no << bit_no) - 2**bit_no
                lower = functools.reduce(lambda a, b: a + b, parts[first : first + 2**bit_no])
                scale = level_scale(near_levels + 1 + bit_no, head_dim)
                near_ref[0, block_no, bit_no] = (lower * scale).astype(bf16)
            else:
                near_ref[0, block_no, bit_no] = jnp.zeros((head_dim, head_dim), bf16)


def forward_kernel(
    length_ref, scale_ref, query_ref, grad_ref, key_ref, value_ref, key_prev_ref, value_prev_ref,
    index_ref, table_ref, gain_ref, near_ref, far_ref,
    mixed_ref, stat_ref, key_all, value_all, *, near_levels,
):
    block_no = pl.program_id(0)
    head_no = pl.program_id(1)
    group, rows, head_dim = key_ref.shape

    @pl.when(block_no == 0)
    def _():
        fill(key_all.at[head_no], key_prev_ref, key_ref)
        fill(value_all.at[head_no], value_prev_ref, value_ref)

    query = query_ref[0]
    span = length_ref[head_no]
    window_scale = scale_ref[head_no]
    row_pos, col_pos = positions(rows)
    offset = row_pos - col_pos
    start = pl.multiple_of(block_no * rows, rows)
    total = jnp.zeros((rows, head_dim), f32)
    for piece_no in range(group):
        key_part = key_all[head_no, pl.ds(start + piece_no * rows, rows)]
        value_part = value_all[head_no, pl.ds(start + piece_no * rows, rows)]
        distance = (group - piece_no) * rows
        scores = dot_nt(query, key_part)
        if distance + rows > WINDOW // 2:
            scores = jnp.where(offset < span - distance, scores, 0.0)
        total = total + dot_nn(scores.astype(bf16), value_part)
    weights = columns_of(lane_weights(lane_indices(index_ref[0]), table_ref))

    def picked(level_no):
        return weights[:, level_no : level_no + 1]

    factor = diagonal_factor(row_pos, col_pos, picked, window_scale, near_levels, head_dim)
    key_part = key_all[head_no, pl.ds(start + group * rows, rows)]
    value_part = value_all[head_no, pl.ds(start + group * rows, rows)]
    prob = (dot_nt(query, key_part) * factor).astype(bf16)
    mixed = dot_nn(prob, value_part) + window_scale * total
    for bit_no in range(group.bit_length() - 1):
        mixed = mixed + picked(near_levels + 1 + bit_no) * dot_nn(query, near_ref[0, 0, bit_no])
    mixed = mixed + picked(LEVELS - 1) * dot_nn(query, far_ref[0])
    mixed_ref[0] = mixed
    scaled = grad_ref[0].astype(f32) * gain_ref[0]
    ones = jnp.ones((8, head_dim), bf16)
    squares = dot_nt(ones, (mixed * mixed).astype(bf16))
    crosses = dot_nt(ones, (scaled * mixed).astype(bf16))
    stats = jnp.where(lax.broadcasted_iota(jnp.int32, squares.shape, 0) < 4, squares, crosses)

    @pl.when(head_no == 0)
    def _():
        stat_ref[0] = stats

    @pl.when(head_no > 0)
    def _():
        stat_ref[0] = stat_ref[0] + stats


def norm_kernel(mixed_ref, grad_ref, stat_ref, gain_ref, out_ref, low_ref, gain_part_ref, *, width):
    block_no = pl.program_id(1)
    stats = columns_of(stat_ref[0])
    inv_rms = lax.rsqrt(stats[:, 0:1] / width + epsilon)
    pull = inv_rms * inv_rms * inv_rms * stats[:, 4:5] / width
    mixed = mixed_ref[0]
    grad = grad_ref[0].astype(f32)
    gain = gain_ref[0]
    normed = mixed * inv_rms
    out_ref[0] = (normed * gain).astype(bf16)
    low_ref[0] = (grad * gain * inv_rms - mixed * pull).astype(bf16)
    part = jnp.sum(grad * normed, axis=0, keepdims=True)

    @pl.when(block_no == 0)
    def _():
        gain_part_ref[0] = part

    @pl.when(block_no > 0)
    def _():
        gain_part_ref[0] = gain_part_ref[0] + part


def query_kernel(
    length_ref, scale_ref, query_ref, low_ref, key_ref, value_ref, key_prev_ref, value_prev_ref,
    index_ref, table_ref, near_ref, far_ref,
    query_grad_ref, table_part_ref, near_grad_ref, far_grad_ref, key_all, value_all, *, near_levels,
):
    head_no = pl.program_id(0)
    block_no = pl.program_id(1)
    group, rows, head_dim = key_ref.shape

    @pl.when(block_no == 0)
    def _():
        fill(key_all, key_prev_ref, key_ref)
        fill(value_all, value_prev_ref, value_ref)

    query = query_ref[0]
    low = low_ref[0]
    span = length_ref[head_no]
    window_scale = scale_ref[head_no]
    row_pos, col_pos = positions(rows)
    offset = row_pos - col_pos
    start = pl.multiple_of(block_no * rows, rows)
    total = jnp.zeros((rows, head_dim), f32)
    for piece_no in range(group):
        key_part = key_all[pl.ds(start + piece_no * rows, rows)]
        value_part = value_all[pl.ds(start + piece_no * rows, rows)]
        distance = (group - piece_no) * rows
        scores = dot_nt(low, value_part)
        if distance + rows > WINDOW // 2:
            scores = jnp.where(offset < span - distance, scores, 0.0)
        total = total + dot_nn(scores.astype(bf16), key_part)
    indices = lane_indices(index_ref[0])
    weights = columns_of(lane_weights(indices, table_ref))

    def picked(level_no):
        return weights[:, level_no : level_no + 1]

    factor = diagonal_factor(row_pos, col_pos, picked, window_scale, near_levels, head_dim)
    key_part = key_all[pl.ds(start + group * rows, rows)]
    value_part = value_all[pl.ds(start + group * rows, rows)]
    prob_grad = dot_nt(low, value_part)
    result = dot_nn((prob_grad * factor).astype(bf16), key_part) + window_scale * total
    pairs = jnp.where(row_pos >= col_pos, dot_nt(query, key_part) * prob_grad, 0.0).astype(bf16)
    leaf_count = rows // BLOCK
    leaf_row = lax.broadcasted_iota(jnp.int32, (8, rows), 0)
    leaf_col = lax.broadcasted_iota(jnp.int32, (8, rows), 1) // BLOCK
    leaf_sums = dot_nt((leaf_row == leaf_col).astype(bf16), pairs)
    level_rows = [jnp.zeros((1, rows), f32) for _ in range(LEVELS)]
    own_leaf = leaf_col[:1]
    for leaf_no in range(leaf_count):
        leaf_sum = leaf_sums[leaf_no : leaf_no + 1]
        apart = own_leaf ^ leaf_no
        level_rows[0] = level_rows[0] + jnp.where(apart == 0, leaf_sum, 0.0)
        for level_no in range(1, near_levels + 1):
            here = (apart >> (level_no - 1)) == 1
            level_rows[level_no] = level_rows[level_no] + jnp.where(here, leaf_sum, 0.0)
    for level_no in range(near_levels + 1):
        level_rows[level_no] = level_rows[level_no] * level_scale(level_no, head_dim)
    ones = jnp.ones((8, head_dim), bf16)
    query_wide = query.astype(f32)
    low_wide = low.astype(f32)
    states = [near_ref[0, 0, bit_no] for bit_no in range(group.bit_length() - 1)] + [far_ref[0]]
    for state_no, state in enumerate(states):
        level_no = near_levels + 1 + state_no
        back = dot_nt(low, state)
        result = result + picked(level_no) * back
        level_rows[level_no] = dot_nt(ones, (query_wide * back).astype(bf16))[:1]
        upstream = (picked(level_no) * low_wide).astype(bf16)
        outer = dot_tn(query, upstream)
        if state_no < len(states) - 1:
            near_grad_ref[0, 0, state_no] = outer
        else:
            @pl.when(block_no == 0)
            def _():
                far_grad_ref[0] = outer

            @pl.when(block_no > 0)
            def _():
                far_grad_ref[0] = far_grad_ref[0] + outer
    query_grad_ref[0] = result.astype(bf16)
    blank = jnp.zeros((8 - LEVELS, rows), f32)
    weight_grad = jnp.concatenate(level_rows + [blank], axis=0)
    lanes = table_part_ref.shape[-1]

    @pl.when(block_no == 0)
    def _():
        table_part_ref[...] = jnp.zeros(table_part_ref.shape, f32)

    for row_no in range(TABLE_ROWS):
        chosen = jnp.where(indices == row_no, weight_grad, 0.0)
        folded = functools.reduce(
            lambda a, b: a + b, [chosen[:, i : i + lanes] for i in range(0, rows, lanes)]
        )
        table_part_ref[0, row_no] = table_part_ref[0, row_no] + folded


def key_kernel(
    length_ref, scale_ref, key_ref, value_ref, query_ref, low_ref, query_next_ref, low_next_ref,
    index_ref, table_ref, near_grad_ref, far_grad_ref,
    key_grad_ref, value_grad_ref, query_all, low_all, *, near_levels,
):
    head_no = pl.program_id(0)
    block_no = pl.program_id(1)
    group, rows, head_dim = query_ref.shape

    @pl.when(block_no == 0)
    def _():
        fill(query_all, query_ref, query_next_ref)
        fill(low_all, low_ref, low_next_ref)

    key = key_ref[0]
    value = value_ref[0]
    span = length_ref[head_no]
    window_scale = scale_ref[head_no]
    row_pos, col_pos = positions(rows)
    offset = col_pos - row_pos
    start = pl.multiple_of(block_no * rows, rows)
    key_total = jnp.zeros((rows, head_dim), f32)
    value_total = jnp.zeros((rows, head_dim), f32)
    for piece_no in range(1, group + 1):
        query_part = query_all[pl.ds(start + piece_no * rows, rows)]
        low_part = low_all[pl.ds(start + piece_no * rows, rows)]
        distance = piece_no * rows
        prob = dot_nt(key, query_part)
        prob_grad = dot_nt(value, low_part)
        if distance + rows > WINDOW // 2:
            inside = offset < span - distance
            prob = jnp.where(inside, prob, 0.0)
            prob_grad = jnp.where(inside, prob_grad, 0.0)
        value_total = value_total + dot_nn(prob.astype(bf16), low_part)
        key_total = key_total + dot_nn(prob_grad.astype(bf16), query_part)
    weights = lane_weights(lane_indices(index_ref[0]), table_ref)

    def picked(level_no):
        return weights[level_no : level_no + 1]

    factor = diagonal_factor(col_pos, row_pos, picked, window_scale, near_levels, head_dim)
    query_part = query_all[pl.ds(start, rows)]
    low_part = low_all[pl.ds(start, rows)]
    prob = (dot_nt(key, query_part) * factor).astype(bf16)
    prob_grad = (dot_nt(value, low_part) * factor).astype(bf16)
    state = far_grad_ref[0]
    for bit_no in range(group.bit_length() - 1):
        first = (block_no >> bit_no | 1) << bit_no
        scale = jnp.where(
            block_no >> bit_no & 1 == 0, level_scale(near_levels + 1 + bit_no, head_dim), 0.0
        )
        for step_no in range(2**bit_no):
            state = state + near_grad_ref[0, first + step_no, bit_no] * scale
    state = state.astype(bf16)
    value_grad = dot_nn(prob, low_part) + window_scale * value_total + dot_nn(key, state)
    key_grad = dot_nn(prob_grad, query_part) + window_scale * key_total + dot_nt(value, state)
    value_grad_ref[0] = value_grad.astype(bf16)
    key_grad_ref[0] = key_grad.astype(bf16)


def grouped_shards(
    query_rows, key_rows, value_rows, norm_gain, level_table, level_index, window_length, out_grad
):
    heads_here, rows, head_dim = query_rows.shape
    group = WINDOW // rows
    heads = heads_here // group
    group_bits = group.bit_length() - 1
    near_levels = (rows // BLOCK).bit_length() - 1
    seq_count = lax.axis_size("seq")
    chunk_bits = (seq_count // group).bit_length() - 1
    seq_index = lax.axis_index("seq")
    member = seq_index & (group - 1)
    width = float(heads_here * lax.axis_size("head") * head_dim)

    def swapped(shard, bits):
        return lax.ppermute(shard, "seq", [(i, i ^ bits) for i in range(seq_count)])

    def regrouped(payload):
        pieces = [
            swapped(lax.dynamic_index_in_dim(payload, member ^ bits, 0), bits)
            for bits in range(1, group)
        ]
        own = lax.dynamic_index_in_dim(payload, member, 0)
        result = lax.dynamic_update_slice_in_dim(jnp.zeros_like(payload), own, member, 0)
        for bits in range(1, group):
            result = lax.dynamic_update_slice_in_dim(result, pieces[bits - 1], member ^ bits, 0)
        return result

    def by_member(tensor):
        return tensor.reshape(group, heads * rows, head_dim)

    index_pad = jnp.pad(level_index.astype(bf16), ((0, 0), (0, 8 - LEVELS)))
    index_pack = index_pad.reshape(rows // 128, 128, 8).transpose(0, 2, 1).reshape(index_rows, 128)
    index_pack = jnp.broadcast_to(index_pack[None], (group, index_rows, 128))
    pair = regrouped(jnp.concatenate([by_member(key_rows), by_member(value_rows)], axis=1))
    rest = regrouped(
        jnp.concatenate([by_member(query_rows), by_member(out_grad), index_pack], axis=1)
    )
    pair_prev = shifted(pair, "seq", group)
    query_next = shifted(rest[:, : heads * rows], "seq", -group)

    first_head = member * heads
    table = lax.dynamic_slice_in_dim(level_table, first_head, heads, 1)
    table = jnp.pad(table.transpose(1, 0, 2), ((0, 0), (0, 0), (0, 8 - LEVELS)))
    table = jnp.broadcast_to(table[..., None], (heads, TABLE_ROWS, 8, 128))
    gain = lax.dynamic_slice_in_dim(norm_gain, first_head, heads, 0)[:, None, :]
    length = lax.dynamic_slice_in_dim(window_length, first_head, heads, 0)
    scale = lax.rsqrt((head_dim * length).astype(f32))

    smem = pl.BlockSpec(memory_space=pltpu.SMEM)
    state_shape = (head_dim, head_dim)
    chunk_shape = (group, heads * rows, head_dim)
    near_shape = (heads, group, group_bits) + state_shape

    def whole(first, head_of):
        return pl.BlockSpec(
            (group, rows, head_dim), lambda *pos: (0, first * heads + head_of(pos), 0)
        )

    def piece(first, head_of, block_of):
        return pl.BlockSpec(
            (1, rows, head_dim), lambda *pos: (block_of(pos), first * heads + head_of(pos), 0)
        )

    def per_head(shape, head_of):
        return pl.BlockSpec((1,) + shape, lambda *pos: (head_of(pos),) + (0,) * len(shape))

    def per_block(shape, head_of, block_of):
        return pl.BlockSpec(
            (1, 1) + shape, lambda *pos: (head_of(pos), block_of(pos)) + (0,) * len(shape)
        )

    def index_spec(block_of):
        return pl.BlockSpec(
            (1, index_rows, 128),
            lambda *pos: (block_of(pos), 2 * heads * rows // index_rows, 0),
        )

    def axis0(pos):
        return pos[0]

    def axis1(pos):
        return pos[1]

    near, total = pl.pallas_call(
        functools.partial(summary_kernel, near_levels=near_levels),
        grid=(heads,),
        in_specs=[whole(0, axis0), whole(1, axis0)],
        out_specs=[
            per_head((group, group_bits) + state_shape, axis0),
            per_head(state_shape, axis0),
        ],
        out_shape=[
            jax.ShapeDtypeStruct(near_shape, bf16),
            jax.ShapeDtypeStruct((heads,) + state_shape, f32),
        ],
        name="summaries",
    )(pair, pair)
    far = jnp.zeros((heads,) + state_shape, f32)
    running = total
    for bit_no in range(chunk_bits):
        partner = swapped(running.astype(bf16), group << bit_no).astype(f32)
        upper = seq_index // group >> bit_no & 1 == 1
        far_scale = level_scale(near_levels + group_bits + 1 + bit_no, head_dim)
        far = far + jnp.where(upper, partner * far_scale, 0.0)
        running = running + partner
    far = far.astype(bf16)

    mixed, stats = pl.pallas_call(
        functools.partial(forward_kernel, near_levels=near_levels),
        grid=(group, heads),
        in_specs=[
            smem,
            smem,
            piece(0, axis1, axis0),
            piece(1, axis1, axis0),
            whole(0, axis1),
            whole(1, axis1),
            whole(0, axis1),
            whole(1, axis1),
            index_spec(axis0),
            per_head((TABLE_ROWS, 8, 128), axis1),
            per_head((1, head_dim), axis1),
            per_block((group_bits,) + state_shape, axis1, axis0),
            per_head(state_shape, axis1),
        ],
        out_specs=[
            piece(0, axis1, axis0),
            pl.BlockSpec((1, 8, rows), lambda *pos: (pos[0], 0, 0)),
        ],
        out_shape=[
            jax.ShapeDtypeStruct(chunk_shape, f32),
            jax.ShapeDtypeStruct((group, 8, rows), f32),
        ],
        scratch_shapes=[
            pltpu.VMEM((heads, 2 * group * rows, head_dim), bf16),
            pltpu.VMEM((heads, 2 * group * rows, head_dim), bf16),
        ],
        name="forward",
    )(length, scale, rest, rest, pair, pair, pair_prev, pair_prev, rest, table, gain, near, far)

    for bit_no in range(group_bits):
        stats = stats + swapped(stats, 1 << bit_no)
    head_count = lax.axis_size("head")
    part = stats
    for step_no in range(1, head_count):
        turn = [(i, (i + step_no) % head_count) for i in range(head_count)]
        stats = stats + lax.ppermute(part, "head", turn)

    layer_out, low, gain_part = pl.pallas_call(
        functools.partial(norm_kernel, width=width),
        grid=(heads, group),
        in_specs=[
            piece(0, axis0, axis1),
            piece(1, axis0, axis1),
            pl.BlockSpec((1, 8, rows), lambda *pos: (pos[1], 0, 0)),
            per_head((1, head_dim), axis0),
        ],
        out_specs=[
            piece(0, axis0, axis1),
            piece(0, axis0, axis1),
            per_head((1, head_dim), axis0),
        ],
        out_shape=[
            jax.ShapeDtypeStruct(chunk_shape, bf16),
            jax.ShapeDtypeStruct(chunk_shape, bf16),
            jax.ShapeDtypeStruct((heads, 1, head_dim), f32),
        ],
        name="norm",
    )(mixed, rest, stats, gain)
    low_next = shifted(low, "seq", -group)

    query_grad, table_part, near_grad, far_part = pl.pallas_call(
        functools.partial(query_kernel, near_levels=near_levels),
        grid=(heads, group),
        in_specs=[
            smem,
            smem,
            piece(0, axis0, axis1),
            piece(0, axis0, axis1),
            whole(0, axis0),
            whole(1, axis0),
            whole(0, axis0),
            whole(1, axis0),
            index_spec(axis1),
            per_head((TABLE_ROWS, 8, 128), axis0),
            per_block((group_bits,) + state_shape, axis0, axis1),
            per_head(state_shape, axis0),
        ],
        out_specs=[
            piece(0, axis0, axis1),
            per_head((TABLE_ROWS, 8, 128), axis0),
            per_block((group_bits,) + state_shape, axis0, axis1),
            per_head(state_shape, axis0),
        ],
        out_shape=[
            jax.ShapeDtypeStruct(chunk_shape, bf16),
            jax.ShapeDtypeStruct((heads, TABLE_ROWS, 8, 128), f32),
            jax.ShapeDtypeStruct(near_shape, f32),
            jax.ShapeDtypeStruct((heads,) + state_shape, f32),
        ],
        scratch_shapes=[
            pltpu.VMEM((2 * group * rows, head_dim), bf16),
            pltpu.VMEM((2 * group * rows, head_dim), bf16),
        ],
        name="query_side",
    )(length, scale, rest, low, pair, pair, pair_prev, pair_prev, rest, table, near, far)

    table_sum = jnp.sum(table_part, axis=-1)
    table_sum = jnp.pad(table_sum, ((0, 0), (0, 0), (0, head_dim - 8)))
    running = jnp.concatenate([far_part, table_sum, gain_part], axis=1)
    far_grad = jnp.zeros((heads,) + state_shape, f32)
    for bit_no in range(chunk_bits):
        partner = swapped(running, group << bit_no)
        lower = seq_index // group >> bit_no & 1 == 0
        far_scale = level_scale(near_levels + group_bits + 1 + bit_no, head_dim)
        far_grad = far_grad + jnp.where(lower, partner[:, :head_dim] * far_scale, 0.0)
        running = running + partner
    small = running[:, head_dim:]

    key_grad, value_grad = pl.pallas_call(
        functools.partial(key_kernel, near_levels=near_levels),
        grid=(heads, group),
        in_specs=[
            smem,
            smem,
            piece(0, axis0, axis1),
            piece(1, axis0, axis1),
            whole(0, axis0),
            whole(0, axis0),
            whole(0, axis0),
            whole(0, axis0),
            index_spec(axis1),
            per_head((TABLE_ROWS, 8, 128), axis0),
            per_head((group, group_bits) + state_shape, axis0),
            per_head(state_shape, axis0),
        ],
        out_specs=[piece(0, axis0, axis1), piece(0, axis0, axis1)],
        out_shape=[jax.ShapeDtypeStruct(chunk_shape, bf16)] * 2,
        scratch_shapes=[
            pltpu.VMEM((2 * group * rows, head_dim), bf16),
            pltpu.VMEM((2 * group * rows, head_dim), bf16),
        ],
        name="key_side",
    )(
        length, scale, pair, pair, rest, low, query_next, low_next, rest, table, near_grad, far_grad
    )

    half = heads * rows
    first_out = regrouped(jnp.concatenate([layer_out, query_grad], axis=1))
    last_out = regrouped(jnp.concatenate([key_grad, value_grad], axis=1))
    small = regrouped(jnp.broadcast_to(small[None], (group,) + small.shape))
    small = small.reshape((heads_here,) + small.shape[2:])

    def by_head(payload):
        return payload.reshape(query_rows.shape)

    return (
        by_head(first_out[:, :half]),
        by_head(first_out[:, half:]),
        by_head(last_out[:, :half]),
        by_head(last_out[:, half:]),
        small[:, :TABLE_ROWS, :LEVELS].transpose(1, 0, 2),
        small[:, TABLE_ROWS],
    )


def fits_groups(heads_here, rows, seq_count):
    group = WINDOW // rows
    levels_fit = (WINDOW // BLOCK).bit_length() + 1 == LEVELS
    return (
        group * rows == WINDOW
        and rows == 2 * 128
        and group == 1 << (group.bit_length() - 1)
        and heads_here % group == 0
        and seq_count % group == 0
        and seq_count == 1 << (seq_count.bit_length() - 1)
        and levels_fit
    )


def shards(query_rows, *others):
    heads_here, rows, _ = query_rows.shape
    if fits_groups(heads_here, rows, lax.axis_size("seq")):
        return grouped_shards(query_rows, *others)
    return wide_shards(query_rows, *others)


def solution(mesh):
    placed = (
        P("head", "seq", None),
        P("head", "seq", None),
        P("head", "seq", None),
        P("head", None),
        P(None, "head", None),
        P("seq", None),
        P("head"),
        P("head", "seq", None),
    )
    return jax.shard_map(
        shards,
        mesh=mesh,
        in_specs=placed,
        out_specs=(
            P("head", "seq", None),
            P("head", "seq", None),
            P("head", "seq", None),
            P("head", "seq", None),
            P(None, "head", None),
            P("head", None),
        ),
        check_vma=False,
    )
```

```python
import functools
import math

import jax
import jax.numpy as jnp
from jax import lax
from jax.experimental import pallas as pl
from jax.experimental.pallas import tpu as pltpu
from jax.sharding import PartitionSpec as P


H = 16
BLOCK = 64
WINDOW = 1024
LEVELS = 6
TABLE_ROWS = 16


epsilon = 1e-06
block_cap = 512


def shifted(block, axis, distance):
    devices = range(lax.axis_size(axis))
    route = [(i - distance, i) for i in devices if i - distance in devices]
    return lax.ppermute(block, axis, route)


def from_partner(shard, axis, bit):
    return lax.ppermute(shard, axis, [(i, i ^ 1 << bit) for i in range(lax.axis_size(axis))])


def contract(pattern, left_side, right_side):
    return jnp.einsum(pattern, left_side, right_side, preferred_element_type=jnp.float32)


def causal_mask():
    row_pos = lax.broadcasted_iota(jnp.int32, (BLOCK, BLOCK), 0)
    col_pos = lax.broadcasted_iota(jnp.int32, (BLOCK, BLOCK), 1)
    return row_pos >= col_pos


def window_mask(block_rows, shift_rows, key_count, span_len):
    query_pos = lax.broadcasted_iota(jnp.int32, (block_rows, key_count), 0)
    key_pos = lax.broadcasted_iota(jnp.int32, (block_rows, key_count), 1)
    offset = query_pos + shift_rows - key_pos
    return (offset >= 0) & (offset < span_len)


def leaf_view(tensor):
    head_count, token_count, head_dim = tensor.shape
    return tensor.reshape(head_count, token_count // BLOCK, BLOCK, head_dim)


def split_level(tensor, group_len):
    head_count, token_count, head_dim = tensor.shape
    return tensor.reshape(head_count, token_count // (2 * group_len), 2, group_len, head_dim)


def level_summary(key_rows, value_rows, group_len):
    lower_sum = contract(
        "hpse,hpsf->hpef",
        split_level(key_rows, group_len)[:, :, 0],
        split_level(value_rows, group_len)[:, :, 0],
    )
    return (lower_sum * (1.0 / math.sqrt(group_len * key_rows.shape[-1]))).astype(jnp.bfloat16)


def level_area(query_rows, summary, group_len):
    upper_half = contract("hpse,hpef->hpsf", split_level(query_rows, group_len)[:, :, 1], summary)
    return jnp.stack([jnp.zeros_like(upper_half), upper_half], axis=2).reshape(query_rows.shape)


def level_grads(query_rows, key_rows, value_rows, summary, upstream, group_len):
    upstream_up = split_level(upstream, group_len)[:, :, 1]
    query_up = contract("hpsf,hpef->hpse", upstream_up, summary)
    summary_grad = contract(
        "hpse,hpsf->hpef", split_level(query_rows, group_len)[:, :, 1], upstream_up
    )
    low_grad = (summary_grad * (1.0 / math.sqrt(group_len * query_rows.shape[-1]))).astype(
        jnp.bfloat16
    )
    key_low = contract("hpsf,hpef->hpse", split_level(value_rows, group_len)[:, :, 0], low_grad)
    value_low = contract("hpse,hpef->hpsf", split_level(key_rows, group_len)[:, :, 0], low_grad)
    blank = jnp.zeros_like(query_up)
    full_shape = query_rows.shape
    return (
        jnp.stack([blank, query_up], axis=2).reshape(full_shape),
        jnp.stack([key_low, blank], axis=2).reshape(full_shape),
        jnp.stack([value_low, blank], axis=2).reshape(full_shape),
    )


def window_head(query_head, key_head, value_head, span_len):
    token_count, head_dim = query_head.shape
    block_rows = min(block_cap, token_count)
    score_scale = lax.rsqrt((head_dim * span_len).astype(jnp.float32))
    inside = window_mask(block_rows, WINDOW, WINDOW + block_rows, span_len)
    scores = contract("qe,ke->qk", query_head, key_head) * score_scale
    prob_low = jnp.where(inside, scores, 0.0).astype(jnp.bfloat16)
    outputs = [contract("qk,ke->qe", prob_low, value_head)]
    return jnp.concatenate(outputs, axis=0)


def window_back_head(query_head, key_head, value_head, grad_head, span_len, keep_from):
    token_count, head_dim = query_head.shape
    block_rows = min(block_cap, token_count)
    score_scale = lax.rsqrt((head_dim * span_len).astype(jnp.float32))
    inside = window_mask(block_rows, WINDOW, WINDOW + block_rows, span_len)
    key_grad = jnp.zeros((WINDOW + token_count - keep_from, head_dim), jnp.float32)
    value_grad = jnp.zeros((WINDOW + token_count - keep_from, head_dim), jnp.float32)
    grad_part = grad_head[0:block_rows]
    scores = contract("qe,ke->qk", query_head, key_head) * score_scale
    prob_low = jnp.where(inside, scores, 0.0).astype(jnp.bfloat16)
    prob_grad = contract("qe,ke->qk", grad_part, value_head)
    score_grad = jnp.where(inside, prob_grad * score_scale, 0.0).astype(jnp.bfloat16)
    query_grad = [contract("qk,ke->qe", score_grad, key_head)]
    skip_cols = max(keep_from, 0)
    target = skip_cols - keep_from
    length_now = WINDOW + block_rows - skip_cols
    key_grad = key_grad.at[target : target + length_now].add(
        contract("qk,qe->ke", score_grad[:, skip_cols:], query_head)
    )
    value_grad = value_grad.at[target : target + length_now].add(
        contract("qk,qe->ke", prob_low, grad_part)
    )
    return (jnp.concatenate(query_grad, axis=0), key_grad, value_grad)


def wide_shards(
    query_rows, key_rows, value_rows, norm_gain, level_table, level_index, window_length, out_grad
):
    heads_here, tok_here, head_dim = query_rows.shape
    seq_index = lax.axis_index("seq")
    seq_levels = lax.axis_size("seq").bit_length() - 1
    local_levels = (tok_here // BLOCK).bit_length() - 1
    reach_count = WINDOW // tok_here
    onehot = (
        level_index[:, :, None] == lax.broadcasted_iota(jnp.int32, (1, 1, TABLE_ROWS), 2)
    ).astype(jnp.float32)
    weights = jnp.einsum("tjk,khj->htj", onehot, level_table, precision=lax.Precision.HIGHEST)

    def weight_of(level_no):
        return weights[:, :, min(level_no, LEVELS - 1)][:, :, None]

    own_pair = jnp.stack([key_rows, value_rows])
    pieces = []
    for step_no in range(reach_count, 0, -1):
        pieces.append(shifted(own_pair, "seq", step_no))
    pieces.append(own_pair)
    wide_pair = jnp.concatenate(pieces, axis=2)
    device_summary = contract("hte,htf->hef", key_rows, value_rows)
    sibling = []
    running = device_summary
    for bit_no in range(seq_levels):
        partner = from_partner(running, "seq", bit_no)
        upper_half = seq_index >> bit_no & 1 == 1
        sibling.append(jnp.where(upper_half, partner, 0.0))
        running = running + partner
    query_leaf = leaf_view(query_rows)
    key_leaf = leaf_view(key_rows)
    value_leaf = leaf_view(value_rows)
    leaf_scale = 1.0 / math.sqrt(BLOCK * head_dim)
    causal = causal_mask()
    leaf_prob = jnp.where(
        causal, contract("hcte,hcse->hcts", query_leaf, key_leaf) * leaf_scale, 0.0
    ).astype(jnp.bfloat16)
    area_list = [contract("hcts,hcse->hcte", leaf_prob, value_leaf).reshape(query_rows.shape)]
    summaries = []
    for level_no in range(1, local_levels + 1):
        group_len = BLOCK * 2 ** (level_no - 1)
        summary = level_summary(key_rows, value_rows, group_len)
        summaries.append(summary)
        area_list.append(level_area(query_rows, summary, group_len))
    for bit_no in range(seq_levels):
        group_len = tok_here * 2**bit_no
        summary = (sibling[bit_no] * (1.0 / math.sqrt(group_len * head_dim))).astype(jnp.bfloat16)
        summaries.append(summary)
        area_list.append(contract("hte,hef->htf", query_rows, summary))
    mixed = lax.map(
        lambda head_items: window_head(head_items[0], head_items[1], head_items[2], head_items[3]),
        (query_rows, wide_pair[0], wide_pair[1], window_length),
    )
    for level_no in range(len(area_list)):
        mixed = mixed + weight_of(level_no) * area_list[level_no]
    grad_full = out_grad.astype(jnp.float32)
    scaled = grad_full * norm_gain[:, None, :]
    square_sum, cross_sum = lax.psum(
        (jnp.sum(mixed * mixed, axis=(0, 2)), jnp.sum(scaled * mixed, axis=(0, 2))), "head"
    )
    inv_rms = lax.rsqrt(square_sum / (H * head_dim) + epsilon)
    layer_out = (mixed * inv_rms[None, :, None] * norm_gain[:, None, :]).astype(jnp.bfloat16)
    mixed_grad = (
        scaled * inv_rms[None, :, None]
        - mixed * (inv_rms**3 * cross_sum / (H * head_dim))[None, :, None]
    )
    gain_part = jnp.sum(grad_full * mixed * inv_rms[None, :, None], axis=1)
    grad_low = mixed_grad.astype(jnp.bfloat16)
    columns = [jnp.zeros((heads_here, tok_here), jnp.float32) for _ in range(LEVELS)]
    for level_no in range(len(area_list)):
        column_no = min(level_no, LEVELS - 1)
        columns[column_no] = columns[column_no] + jnp.sum(mixed_grad * area_list[level_no], axis=2)
    upstream_leaf = leaf_view((weight_of(0) * mixed_grad).astype(jnp.bfloat16))
    prob_grad = contract("hcte,hcse->hcts", upstream_leaf, value_leaf)
    score_grad = jnp.where(causal, prob_grad * leaf_scale, 0.0).astype(jnp.bfloat16)
    query_grad = contract("hcts,hcse->hcte", score_grad, key_leaf).reshape(query_rows.shape)
    key_grad = contract("hcts,hcte->hcse", score_grad, query_leaf).reshape(query_rows.shape)
    value_grad = contract("hcts,hcte->hcse", leaf_prob, upstream_leaf).reshape(query_rows.shape)
    for level_no in range(1, local_levels + 1):
        group_len = BLOCK * 2 ** (level_no - 1)
        upstream = (weight_of(level_no) * mixed_grad).astype(jnp.bfloat16)
        query_part, key_part, value_part = level_grads(
            query_rows, key_rows, value_rows, summaries[level_no - 1], upstream, group_len
        )
        query_grad = query_grad + query_part
        key_grad = key_grad + key_part
        value_grad = value_grad + value_part
    summary_grads = []
    for bit_no in range(seq_levels):
        level_no = local_levels + 1 + bit_no
        upstream = (weight_of(level_no) * mixed_grad).astype(jnp.bfloat16)
        query_grad = query_grad + contract("htf,hef->hte", upstream, summaries[level_no - 1])
        group_len = tok_here * 2**bit_no
        partial_value = contract("hte,htf->hef", query_rows, upstream) * (
            1.0 / math.sqrt(group_len * head_dim)
        )
        upper_half = seq_index >> bit_no & 1 == 1
        summary_grads.append(jnp.where(upper_half, partial_value, 0.0))
    pending = jnp.stack(summary_grads)
    for bit_no in range(seq_levels):
        partner = from_partner(pending[bit_no:], "seq", bit_no)
        lower_half = seq_index >> bit_no & 1 == 0
        received = jnp.where(lower_half, partner[0], 0.0).astype(jnp.bfloat16)
        key_grad = key_grad + contract("htf,hef->hte", value_rows, received)
        value_grad = value_grad + contract("hte,hef->htf", key_rows, received)
        pending = jnp.concatenate(
            [pending[: bit_no + 1], pending[bit_no + 1 :] + partner[1:]], axis=0
        )
    keep_from = 0
    window_query, window_key, window_value = lax.map(
        lambda head_items: window_back_head(
            head_items[0], head_items[1], head_items[2], head_items[3], head_items[4], keep_from
        ),
        (query_rows, wide_pair[0], wide_pair[1], grad_low, window_length),
    )
    query_grad = query_grad + window_query
    key_grad = key_grad + window_key[:, WINDOW:]
    value_grad = value_grad + window_value[:, WINDOW:]
    for step_no in range(1, reach_count + 1):
        first_row = (reach_count - step_no) * tok_here
        piece = jnp.stack(
            [
                window_key[:, first_row : first_row + tok_here],
                window_value[:, first_row : first_row + tok_here],
            ]
        )
        arrived = shifted(piece.astype(jnp.bfloat16), "seq", -step_no).astype(piece.dtype)
        key_grad = key_grad + arrived[0]
        value_grad = value_grad + arrived[1]
    weight_grad = jnp.stack(columns, axis=-1)
    table_part = jnp.einsum("tjk,htj->khj", onehot, weight_grad, precision=lax.Precision.HIGHEST)
    table_grad, gain_grad = lax.psum((table_part, gain_part), "seq")
    return (
        layer_out,
        query_grad.astype(jnp.bfloat16),
        key_grad.astype(jnp.bfloat16),
        value_grad.astype(jnp.bfloat16),
        table_grad,
        gain_grad,
    )


f32 = jnp.float32
bf16 = jnp.bfloat16
index_rows = 16
kernel_vmem = 20 * 2**20


def dot_nn(left, right):
    return lax.dot_general(left, right, (((1,), (0,)), ((), ())), preferred_element_type=f32)


def dot_nt(left, right):
    return lax.dot_general(left, right, (((1,), (1,)), ((), ())), preferred_element_type=f32)


def dot_tn(left, right):
    return lax.dot_general(left, right, (((0,), (0,)), ((), ())), preferred_element_type=f32)


def added(parts):
    return functools.reduce(lambda a, b: a + b, parts)


def level_scale(level_no, head_dim):
    return 1.0 / math.sqrt(BLOCK * 2 ** max(level_no - 1, 0) * head_dim)


def lane_indices(index_block):
    rows = index_block.astype(f32)
    return jnp.concatenate([rows[:8], rows[8:]], axis=1)


def lane_weights(indices, table_ref):
    weights = jnp.zeros(indices.shape, f32)
    wide = indices.shape[1] // table_ref.shape[-1]
    for row_no in range(TABLE_ROWS):
        row = jnp.concatenate([table_ref[0, row_no]] * wide, axis=1)
        weights = jnp.where(indices == row_no, row, weights)
    return weights


def positions(rows, cols):
    row_pos = lax.broadcasted_iota(jnp.int32, (rows, cols), 0)
    col_pos = lax.broadcasted_iota(jnp.int32, (rows, cols), 1)
    return row_pos, col_pos


def diagonal_factor(query_pos, key_pos, picked, window_scale, near_levels, head_dim):
    shift = BLOCK.bit_length() - 1
    apart = (query_pos >> shift) ^ (key_pos >> shift)
    factor = picked(0) * level_scale(0, head_dim) + window_scale
    for level_no in range(1, near_levels + 1):
        factor = jnp.where(
            apart >= 2 ** (level_no - 1),
            picked(level_no) * level_scale(level_no, head_dim) + window_scale,
            factor,
        )
    return jnp.where(query_pos >= key_pos, factor, 0.0)


def place(target, first_block, piece_refs, member):
    rows = piece_refs[0].shape[0]
    for bits, piece_ref in enumerate(piece_refs):
        start = pl.multiple_of((first_block + (member ^ bits)) * rows, rows)
        target[pl.ds(start, rows)] = piece_ref[...]


def copy_all(pairs, semaphore):
    copies = [pltpu.make_async_copy(a, b, semaphore.at[i]) for i, (a, b) in enumerate(pairs)]
    for copy in copies:
        copy.start()
    for copy in copies:
        copy.wait()


def pack_kernel(member_ref, *refs, group, extra):
    *refs, semaphore = refs
    sources, pieces = refs[:-group], refs[-group:]
    heads = sources[0].shape[0] // group
    rows = sources[0].shape[1]
    pairs = []
    for bits, piece in enumerate(pieces):
        for source_no, source in enumerate(sources[: len(sources) - extra]):
            for head_no in range(heads):
                first = (source_no * heads + head_no) * rows
                block = source.at[(member_ref[0] ^ bits) * heads + head_no]
                pairs.append((block, piece.at[pl.ds(first, rows)]))
        if extra:
            first = (len(sources) - 1) * heads * rows
            pairs.append((sources[-1], piece.at[pl.ds(first, sources[-1].shape[0])]))
    copy_all(pairs, semaphore)


def arrange_kernel(member_ref, *refs, group):
    pieces, targets = refs[:group], refs[group:]
    for bits, piece in enumerate(pieces):
        first = 0
        for target in targets:
            count = target.shape[1]
            target[member_ref[0] ^ bits] = piece[first : first + count]
            first += count


def unpack_kernel(member_ref, *refs, group, head_stride, kind_stride):
    *refs, semaphore = refs
    pieces, outs = refs[:group], refs[group:]
    heads = outs[0].shape[0] // group
    rows = outs[0].shape[1]
    pairs = []
    for bits, piece in enumerate(pieces):
        for head_no in range(heads):
            for kind, out in enumerate(outs):
                first = (head_no * head_stride + kind * kind_stride) * rows
                target = out.at[(member_ref[0] ^ bits) * heads + head_no]
                pairs.append((piece.at[pl.ds(first, rows)], target))
    copy_all(pairs, semaphore)


def window_reach(span, rows):
    whole = span // rows
    return whole, span - whole * rows


def window_state(blocks, whole, steps):
    state = blocks[0]
    for step_no in range(1, steps):
        state = state + blocks[step_no] * jnp.where(whole > step_no + 1, 1.0, 0.0)
    return state


def summary_kernel(member_ref, *refs, group, near_levels):
    key_refs, value_refs = refs[:group], refs[group : 2 * group]
    near_ref, block_ref, total_ref = refs[2 * group : 2 * group + 3]
    key_all, value_all = refs[2 * group + 3 :]
    rows, head_dim = key_refs[0].shape
    member = member_ref[0]
    place(key_all, 0, key_refs, member)
    place(value_all, 0, value_refs, member)
    parts = [
        dot_tn(key_all[i * rows : (i + 1) * rows], value_all[i * rows : (i + 1) * rows])
        for i in range(group)
    ]
    total_ref[0] = added(parts)
    for block_no in range(group):
        block_ref[0, block_no] = parts[block_no]
        for bit_no in range(group.bit_length() - 1):
            if block_no >> bit_no & 1:
                first = (block_no >> bit_no << bit_no) - 2**bit_no
                scale = level_scale(near_levels + 1 + bit_no, head_dim)
                lower = added(parts[first : first + 2**bit_no]) * scale
                near_ref[0, block_no, bit_no] = lower.astype(bf16)
            else:
                near_ref[0, block_no, bit_no] = jnp.zeros((head_dim, head_dim), bf16)


def load_window(member, own_refs, prev_refs, target):
    group = len(own_refs)
    rows, head_dim = own_refs[0].shape
    target[:rows] = jnp.zeros((rows, head_dim), bf16)
    place(target, 1, prev_refs, member)
    place(target, 1 + group, own_refs, member)


def forward_kernel(member_ref, length_ref, scale_ref, last_scale_ref, *refs, group, near_levels):
    key_refs, value_refs = refs[:group], refs[group : 2 * group]
    key_prev, value_prev = refs[2 * group : 3 * group], refs[3 * group : 4 * group]
    (
        query_ref, grad_ref, index_ref, table_ref, gain_ref, near_ref, block_ref, far_ref,
        mixed_ref, stat_ref, state_ref, far_out_ref, key_all, value_all,
    ) = refs[4 * group :]
    head_no = pl.program_id(0)
    _, rows, head_dim = query_ref.shape
    member = member_ref[0]
    load_window(member, key_refs, key_prev, key_all)
    load_window(member, value_refs, value_prev, value_all)
    whole, part = window_reach(length_ref[head_no], rows)
    window_scale = scale_ref[head_no]
    blocks = [
        dot_tn(key_all[i * rows : (i + 1) * rows], value_all[i * rows : (i + 1) * rows])
        for i in range(1, group + 1)
    ]
    far = (far_ref[0] + added(blocks) * last_scale_ref[0]).astype(bf16)
    far_out_ref[0] = far
    blocks = blocks[1:] + [block_ref[0, i] for i in range(group - 1)]
    stat_rows = []
    row_pos, col_pos = positions(rows, rows)
    edge_row, edge_col = positions(rows, 2 * rows)
    edge_mask = edge_row - edge_col < part - rows
    ones = jnp.ones((8, head_dim), bf16)
    for block_no in range(group):
        query = query_ref[block_no]
        start = pl.multiple_of((block_no + group - whole) * rows, rows)
        scores = dot_nt(query, key_all[pl.ds(start, 2 * rows)])
        edge = jnp.where(edge_mask, scores, 0.0).astype(bf16)
        total = dot_nn(edge, value_all[pl.ds(start, 2 * rows)])
        recent = blocks[block_no : block_no + group - 1][::-1]
        state = window_state(recent, whole, group - 1) * window_scale
        state = state.astype(bf16)
        state_ref[0, block_no] = state
        weights = jnp.transpose(lane_weights(lane_indices(index_ref[block_no]), table_ref))

        def picked(level_no):
            return weights[:, level_no : level_no + 1]

        factor = diagonal_factor(row_pos, col_pos, picked, window_scale, near_levels, head_dim)
        own = slice((1 + group + block_no) * rows, (2 + group + block_no) * rows)
        prob = (dot_nt(query, key_all[own]) * factor).astype(bf16)
        mixed = dot_nn(prob, value_all[own]) + window_scale * total + dot_nn(query, state)
        for bit_no in range(group.bit_length() - 1):
            if block_no >> bit_no & 1:
                area = dot_nn(query, near_ref[0, block_no, bit_no])
                mixed = mixed + picked(near_levels + 1 + bit_no) * area
        mixed = mixed + picked(LEVELS - 1) * dot_nn(query, far)
        mixed_ref[block_no] = mixed
        scaled = grad_ref[block_no].astype(f32) * gain_ref[0]
        stat_rows.append(dot_nt(ones, (mixed * mixed).astype(bf16))[:1])
        stat_rows.append(dot_nt(ones, (scaled * mixed).astype(bf16))[:1])
    stats = jnp.concatenate(stat_rows, axis=0)

    @pl.when(head_no == 0)
    def _():
        stat_ref[...] = stats

    @pl.when(head_no > 0)
    def _():
        stat_ref[...] = stat_ref[...] + stats


def norm_kernel(member_ref, mixed_ref, grad_ref, gain_ref, *refs, group, width):
    stat_refs, out_refs = refs[:group], refs[group : 2 * group]
    low_ref, gain_part_ref, out_all = refs[2 * group :]
    gain = gain_ref[0]
    stats = jnp.transpose(added([stat_ref[...] for stat_ref in stat_refs]))
    parts = []
    for block_no in range(group):
        inv_rms = lax.rsqrt(stats[:, 2 * block_no : 2 * block_no + 1] / width + epsilon)
        pull = inv_rms * inv_rms * inv_rms * stats[:, 2 * block_no + 1 : 2 * block_no + 2] / width
        mixed = mixed_ref[block_no]
        grad = grad_ref[block_no].astype(f32)
        normed = mixed * inv_rms
        out_all[block_no] = (normed * gain).astype(bf16)
        low_ref[block_no] = (grad * gain * inv_rms - mixed * pull).astype(bf16)
        parts.append(jnp.sum(grad * normed, axis=0, keepdims=True))
    gain_part_ref[0] = added(parts)
    for bits, out_ref in enumerate(out_refs):
        out_ref[...] = out_all[member_ref[0] ^ bits]


def far_grad_kernel(query_ref, low_ref, index_ref, table_ref, far_grad_ref):
    parts = []
    for block_no in range(query_ref.shape[0]):
        weights = jnp.transpose(lane_weights(lane_indices(index_ref[block_no]), table_ref))
        low = weights[:, LEVELS - 1 : LEVELS] * low_ref[block_no].astype(f32)
        parts.append(dot_tn(query_ref[block_no], low.astype(bf16)))
    far_grad_ref[0] = added(parts).astype(bf16)


def query_kernel(member_ref, length_ref, scale_ref, *refs, group, near_levels):
    key_refs, value_refs = refs[:group], refs[group : 2 * group]
    key_prev, value_prev = refs[2 * group : 3 * group], refs[3 * group : 4 * group]
    (
        query_ref, low_ref, index_ref, table_ref, near_ref, state_ref, far_ref, gain_part_ref,
    ) = refs[4 * group : 4 * group + 8]
    out_refs = refs[5 * group + 8 : 6 * group + 8]
    near_grad_ref, sums_ref, key_all, value_all, out_all = refs[6 * group + 8 :]
    head_no = pl.program_id(0)
    _, rows, head_dim = query_ref.shape
    member = member_ref[0]
    load_window(member, key_refs, key_prev, key_all)
    load_window(member, value_refs, value_prev, value_all)
    whole, part = window_reach(length_ref[head_no], rows)
    window_scale = scale_ref[head_no]
    row_pos, col_pos = positions(rows, rows)
    edge_row, edge_col = positions(rows, 2 * rows)
    edge_mask = edge_row - edge_col < part - rows
    ones = jnp.ones((8, head_dim), bf16)
    leaf_row = lax.broadcasted_iota(jnp.int32, (8, rows), 0)
    leaf_col = lax.broadcasted_iota(jnp.int32, (8, rows), 1) >> (BLOCK.bit_length() - 1)
    leaf_pick = jnp.where(leaf_row == leaf_col, 1.0, 0.0).astype(bf16)
    own_leaf = leaf_col[:1]
    lanes = table_ref.shape[-1]
    table_parts = [jnp.zeros((8, lanes), f32) for _ in range(TABLE_ROWS)]
    for block_no in range(group):
        query = query_ref[block_no]
        low = low_ref[block_no]
        start = pl.multiple_of((block_no + group - whole) * rows, rows)
        scores = dot_nt(low, value_all[pl.ds(start, 2 * rows)])
        edge = jnp.where(edge_mask, scores, 0.0).astype(bf16)
        total = dot_nn(edge, key_all[pl.ds(start, 2 * rows)])
        indices = lane_indices(index_ref[block_no])
        weights = jnp.transpose(lane_weights(indices, table_ref))

        def picked(level_no):
            return weights[:, level_no : level_no + 1]

        factor = diagonal_factor(row_pos, col_pos, picked, window_scale, near_levels, head_dim)
        own = slice((1 + group + block_no) * rows, (2 + group + block_no) * rows)
        prob_grad = dot_nt(low, value_all[own])
        result = dot_nn((prob_grad * factor).astype(bf16), key_all[own])
        result = result + window_scale * total + dot_nt(low, state_ref[0, block_no])
        scores = dot_nt(query, key_all[own])
        pairs = jnp.where(row_pos >= col_pos, scores * prob_grad, 0.0).astype(bf16)
        leaf_sums = dot_nt(leaf_pick, pairs)
        level_rows = [jnp.zeros((1, rows), f32) for _ in range(8)]
        for leaf_no in range(rows // BLOCK):
            leaf_sum = leaf_sums[leaf_no : leaf_no + 1]
            apart = own_leaf ^ leaf_no
            level_rows[0] = level_rows[0] + jnp.where(apart == 0, leaf_sum, 0.0)
            for level_no in range(1, near_levels + 1):
                here = (apart >> (level_no - 1)) == 1
                level_rows[level_no] = level_rows[level_no] + jnp.where(here, leaf_sum, 0.0)
        for level_no in range(near_levels + 1):
            level_rows[level_no] = level_rows[level_no] * level_scale(level_no, head_dim)
        query_wide = query.astype(f32)
        low_wide = low.astype(f32)
        for level_no in range(near_levels + 1, LEVELS):
            bit_no = level_no - near_levels - 1
            last = level_no == LEVELS - 1
            if not last and not block_no >> bit_no & 1:
                continue
            back = dot_nt(low, far_ref[0] if last else near_ref[0, block_no, bit_no])
            result = result + picked(level_no) * back
            level_rows[level_no] = dot_nt(ones, (query_wide * back).astype(bf16))[:1]
            if not last:
                upstream = (picked(level_no) * low_wide).astype(bf16)
                near_grad_ref[0, block_no, bit_no] = dot_tn(query, upstream)
        out_all[block_no] = result.astype(bf16)
        weight_grad = jnp.concatenate(level_rows, axis=0)
        for row_no in range(TABLE_ROWS):
            chosen = jnp.where(indices == row_no, weight_grad, 0.0)
            folded = added([chosen[:, i : i + lanes] for i in range(0, rows, lanes)])
            table_parts[row_no] = table_parts[row_no] + folded
    table_part = jnp.concatenate(table_parts, axis=0)
    table_high = table_part.astype(bf16)
    table_low = (table_part - table_high.astype(f32)).astype(bf16)
    lane_sums = dot_nt(ones, table_high) + dot_nt(ones, table_low)
    for bits, out_ref in enumerate(out_refs):
        out_ref[...] = out_all[member ^ bits]
    heads = pl.num_programs(0)
    row_no = lax.broadcasted_iota(jnp.int32, sums_ref.shape, 0)
    first = (member * heads + head_no) * 2

    @pl.when(head_no == 0)
    def _():
        sums_ref[...] = jnp.zeros(sums_ref.shape, f32)

    sums = jnp.where(row_no == first, lane_sums[:1], sums_ref[...])
    sums_ref[...] = jnp.where(row_no == first + 1, gain_part_ref[0], sums)


def key_kernel(member_ref, length_ref, scale_ref, *refs, group, near_levels):
    key_refs, value_refs = refs[:group], refs[group : 2 * group]
    (
        query_ref, low_ref, query_next_ref, low_next_ref, index_ref, table_ref, near_grad_ref,
        far_grad_ref,
    ) = refs[2 * group : 2 * group + 8]
    out_refs = refs[2 * group + 8 : 3 * group + 8]
    key_all, value_all, query_all, low_all, out_all = refs[3 * group + 8 :]
    head_no = pl.program_id(0)
    _, rows, head_dim = query_ref.shape
    member = member_ref[0]
    place(key_all, 0, key_refs, member)
    place(value_all, 0, value_refs, member)
    for target, first_ref, second_ref in (
        (query_all, query_ref, query_next_ref),
        (low_all, low_ref, low_next_ref),
    ):
        for i in range(group):
            target[i * rows : (i + 1) * rows] = first_ref[i]
            target[(group + i) * rows : (group + i + 1) * rows] = second_ref[i]
        target[2 * group * rows :] = jnp.zeros((rows, head_dim), bf16)
    whole, part = window_reach(length_ref[head_no], rows)
    window_scale = scale_ref[head_no]
    blocks = [
        dot_tn(query_all[i * rows : (i + 1) * rows], low_all[i * rows : (i + 1) * rows])
        for i in range(1, 2 * group - 1)
    ]
    row_pos, col_pos = positions(rows, rows)
    edge_row, edge_col = positions(rows, 2 * rows)
    edge_mask = edge_col - edge_row < part
    for block_no in range(group):
        own = slice(block_no * rows, (block_no + 1) * rows)
        key = key_all[own]
        value = value_all[own]
        start = pl.multiple_of((block_no + whole) * rows, rows)
        query_part = query_all[pl.ds(start, 2 * rows)]
        low_part = low_all[pl.ds(start, 2 * rows)]
        prob = jnp.where(edge_mask, dot_nt(key, query_part), 0.0).astype(bf16)
        prob_grad = jnp.where(edge_mask, dot_nt(value, low_part), 0.0).astype(bf16)
        value_total = dot_nn(prob, low_part)
        key_total = dot_nn(prob_grad, query_part)
        weights = lane_weights(lane_indices(index_ref[block_no]), table_ref)

        def picked(level_no):
            return weights[level_no : level_no + 1]

        factor = diagonal_factor(col_pos, row_pos, picked, window_scale, near_levels, head_dim)
        prob = (dot_nt(key, query_all[own]) * factor).astype(bf16)
        prob_grad = (dot_nt(value, low_all[own]) * factor).astype(bf16)
        state = window_state(blocks[block_no : block_no + group - 1], whole, group - 1)
        state = state * window_scale + far_grad_ref[0]
        for bit_no in range(group.bit_length() - 1):
            if not block_no >> bit_no & 1:
                first = (block_no >> bit_no | 1) << bit_no
                upper = [near_grad_ref[0, first + i, bit_no] for i in range(2**bit_no)]
                state = state + added(upper) * level_scale(near_levels + 1 + bit_no, head_dim)
        state = state.astype(bf16)
        value_grad = dot_nn(prob, low_all[own]) + window_scale * value_total + dot_nn(key, state)
        key_grad = dot_nn(prob_grad, query_all[own]) + window_scale * key_total
        key_grad = key_grad + dot_nt(value, state)
        out_all[block_no, :rows] = key_grad.astype(bf16)
        out_all[block_no, rows:] = value_grad.astype(bf16)
    for bits, out_ref in enumerate(out_refs):
        out_ref[...] = out_all[member ^ bits]


def grouped_shards(
    query_rows, key_rows, value_rows, norm_gain, level_table, level_index, window_length, out_grad
):
    heads_here, rows, head_dim = query_rows.shape
    group = WINDOW // rows
    heads = heads_here // group
    group_bits = group.bit_length() - 1
    near_levels = (rows // BLOCK).bit_length() - 1
    seq_count = lax.axis_size("seq")
    chunk_bits = (seq_count // group).bit_length() - 1
    seq_index = lax.axis_index("seq")
    member = seq_index & (group - 1)
    member_arg = member.astype(jnp.int32).reshape(1)
    head_count = lax.axis_size("head")
    width = float(heads_here * head_count * head_dim)

    def swapped(shard, bits):
        return lax.ppermute(shard, "seq", [(i, i ^ bits) for i in range(seq_count)])

    def moved(shard, distance):
        return shifted(shard, "seq", distance)

    def exchanged(pieces):
        return list(pieces[:1]) + [swapped(pieces[bits], bits) for bits in range(1, group)]

    smem = pl.BlockSpec(memory_space=pltpu.SMEM)
    vmem = pl.BlockSpec(memory_space=pltpu.VMEM)
    hbm = pl.BlockSpec(memory_space=pltpu.HBM)

    def whole_call(kernel, in_specs, outs, copies, *args):
        return pl.pallas_call(
            kernel,
            in_specs=in_specs,
            out_specs=[spec for spec, _, _ in outs],
            out_shape=[jax.ShapeDtypeStruct(shape, dtype) for _, shape, dtype in outs],
            scratch_shapes=[pltpu.SemaphoreType.DMA((copies,))] if copies else [],
            compiler_params=pltpu.CompilerParams(vmem_limit_bytes=kernel_vmem),
        )(*args)

    piece_shape = (2 * heads * rows, head_dim)
    rest_shape = (2 * heads * rows + index_rows, head_dim)
    chunk_shape = (group, heads * rows, head_dim)
    index_shape = (group, index_rows, head_dim)
    pair = whole_call(
        functools.partial(pack_kernel, group=group, extra=0),
        [smem, hbm, hbm], [(vmem, piece_shape, bf16)] * group, 2 * heads * group,
        member_arg, key_rows, value_rows,
    )
    index_pad = jnp.pad(level_index.astype(bf16), ((0, 0), (0, 8 - LEVELS)))
    index_pack = index_pad.reshape(rows // 128, 128, 8).transpose(0, 2, 1).reshape(index_rows, 128)
    rest = whole_call(
        functools.partial(pack_kernel, group=group, extra=1),
        [smem, hbm, hbm, hbm], [(vmem, rest_shape, bf16)] * group, (2 * heads + 1) * group,
        member_arg, query_rows, out_grad, index_pack,
    )
    pair = exchanged(pair)
    pair_prev = [moved(piece, group) for piece in pair]
    rest = exchanged(rest)
    query, grad, index = whole_call(
        functools.partial(arrange_kernel, group=group), [smem] + [vmem] * group,
        [(vmem, chunk_shape, bf16), (vmem, chunk_shape, bf16), (vmem, index_shape, bf16)], 0,
        member_arg, *rest,
    )
    query_next = moved(query, -group)

    first_head = member * heads
    table = lax.dynamic_slice_in_dim(level_table, first_head, heads, 1)
    table = jnp.pad(table.transpose(1, 0, 2), ((0, 0), (0, 0), (0, 8 - LEVELS)))
    table = jnp.broadcast_to(table[..., None], (heads, TABLE_ROWS, 8, 128))
    gain = lax.dynamic_slice_in_dim(norm_gain, first_head, heads, 0)[:, None, :]
    length = lax.dynamic_slice_in_dim(window_length, first_head, heads, 0)
    scale = lax.rsqrt((head_dim * length).astype(f32))

    chunk_no = seq_index // group

    def far_scale(other):
        apart = chunk_no ^ other
        result = jnp.full((), level_scale(near_levels + group_bits + 1, head_dim), f32)
        for bit_no in range(1, chunk_bits):
            scale_here = level_scale(near_levels + group_bits + 1 + bit_no, head_dim)
            result = jnp.where(apart >= 1 << bit_no, scale_here, result)
        return result

    state_shape = (head_dim, head_dim)
    states_shape = (heads,) + state_shape
    near_shape = (heads, group, group_bits) + state_shape
    block_states = (heads, group) + state_shape

    def whole(first):
        return pl.BlockSpec((group, rows, head_dim), lambda h: (0, first * heads + h, 0))

    def each(first):
        return [pl.BlockSpec((rows, head_dim), lambda h: (first * heads + h, 0))] * group

    def per_head(shape):
        return pl.BlockSpec((1,) + shape[1:], lambda h: (h,) + (0,) * (len(shape) - 1))

    def fixed(shape):
        return pl.BlockSpec(shape, lambda h: (0,) * len(shape))

    index_spec = fixed(index_shape)
    table_spec = per_head(table.shape)
    stat_shape = (2 * group, rows)

    def run(kernel, cost, in_specs, outs, scratch, aliases, *args):
        return pl.pallas_call(
            kernel,
            grid=(heads,),
            in_specs=in_specs,
            out_specs=[spec for spec, _, _ in outs],
            out_shape=[jax.ShapeDtypeStruct(shape, dtype) for _, shape, dtype in outs],
            scratch_shapes=[pltpu.VMEM(shape, bf16) for shape in scratch],
            input_output_aliases=aliases,
            cost_estimate=pl.CostEstimate(
                flops=int(cost * 1e9), transcendentals=0, bytes_accessed=4 * 2**20
            ),
            compiler_params=pltpu.CompilerParams(vmem_limit_bytes=kernel_vmem),
        )(*args)

    sizes = dict(group=group, near_levels=near_levels)
    chunk_rows = (group * rows, head_dim)
    window_rows = ((2 * group + 1) * rows, head_dim)
    results = (group, rows, head_dim)
    near, block_sums, total = run(
        functools.partial(summary_kernel, **sizes), 0.5,
        [smem] + each(0) + each(1),
        [
            (per_head(near_shape), near_shape, bf16),
            (per_head(block_states), block_states, f32),
            (per_head(states_shape), states_shape, f32),
        ],
        [chunk_rows] * 2, {}, member_arg, *pair, *pair,
    )
    total = total.astype(bf16)
    far = jnp.zeros(states_shape, f32)
    for step_no in range(2, 1 << chunk_bits):
        other = moved(total, step_no * group).astype(f32)
        far = far + other * far_scale(chunk_no - step_no)
    last_scale = far_scale(chunk_no - 1).reshape(1)
    far_spec = per_head(states_shape)

    mixed, stats, states, far = run(
        functools.partial(forward_kernel, **sizes), 3,
        [smem] * 4 + each(0) + each(1) + each(0) + each(1)
        + [
            whole(0), whole(0), index_spec, table_spec, per_head(gain.shape),
            per_head(near_shape), per_head(block_states), far_spec,
        ],
        [
            (whole(0), chunk_shape, f32),
            (fixed(stat_shape), stat_shape, f32),
            (per_head(block_states), block_states, bf16),
            (far_spec, states_shape, bf16),
        ],
        [window_rows] * 2, {},
        member_arg, length, scale, last_scale, *pair, *pair, *pair_prev, *pair_prev,
        query, grad, index, table, gain, near, block_sums, far,
    )

    part = stats
    for step_no in range(1, head_count):
        turn = [(i, (i + step_no) % head_count) for i in range(head_count)]
        stats = stats + lax.ppermute(part, "head", turn)
    stat_parts = [stats] + [swapped(stats, bits) for bits in range(1, group)]

    out_pieces = [(each(0)[0], piece_shape, bf16)] * group
    *first_out, low, gain_part = run(
        functools.partial(norm_kernel, group=group, width=width), 0.6,
        [smem, whole(0), whole(0), per_head(gain.shape)] + [fixed(stat_shape)] * group,
        out_pieces + [(whole(0), chunk_shape, bf16), (per_head(gain.shape), gain.shape, f32)],
        [results], {}, member_arg, mixed, grad, gain, *stat_parts,
    )
    low_next = moved(low, -group)
    (far_part,) = run(
        far_grad_kernel, 0.3,
        [whole(0), whole(0), index_spec, table_spec], [(far_spec, states_shape, bf16)],
        [], {}, query, low, index, table,
    )
    far_grad = jnp.zeros(states_shape, f32)
    for step_no in range(1, 1 << chunk_bits):
        other = moved(far_part, -step_no * group).astype(f32)
        far_grad = far_grad + other * far_scale(chunk_no + step_no)

    args = (
        member_arg, length, scale, *pair, *pair, *pair_prev, *pair_prev,
        query, low, index, table, near, states, far, gain_part, *first_out,
    )
    sums_shape = (2 * heads_here, head_dim)
    *first_out, near_grad, sums = run(
        functools.partial(query_kernel, **sizes), 3,
        [smem] * 3 + each(0) + each(1) + each(0) + each(1)
        + [
            whole(0), whole(0), index_spec, table_spec, per_head(near_shape),
            per_head(block_states), far_spec, per_head(gain.shape),
        ]
        + [pl.BlockSpec(memory_space=pl.ANY)] * group,
        [(each(1)[0], piece_shape, bf16)] * group
        + [(per_head(near_shape), near_shape, f32), (fixed(sums_shape), sums_shape, f32)],
        [window_rows] * 2 + [results],
        {len(args) - group + bits: bits for bits in range(group)}, *args,
    )
    first_out = exchanged(first_out)

    pair_out = pl.BlockSpec((2 * rows, head_dim), lambda h: (h, 0))
    last_out = run(
        functools.partial(key_kernel, **sizes), 4,
        [smem] * 3 + each(0) + each(1)
        + [
            whole(0), whole(0), whole(0), whole(0), index_spec, table_spec,
            per_head(near_shape), far_spec,
        ],
        [(pair_out, piece_shape, bf16)] * group,
        [chunk_rows] * 2 + [window_rows] * 2 + [(group, 2 * rows, head_dim)], {},
        member_arg, length, scale, *pair, *pair,
        query, low, query_next, low_next, index, table, near_grad, far_grad,
    )
    last_out = exchanged(last_out)

    for step_no in range(chunk_bits + group_bits):
        bit_no = (step_no + group_bits) % (chunk_bits + group_bits)
        sums = sums + swapped(sums, 1 << bit_no)
    sums = sums.reshape(heads_here, 2, head_dim)
    table_grad = sums[:, 0].reshape(heads_here, TABLE_ROWS, 8)[:, :, :LEVELS]

    def unpacked(pieces, head_stride, kind_stride):
        return whole_call(
            functools.partial(
                unpack_kernel, group=group, head_stride=head_stride, kind_stride=kind_stride
            ),
            [smem] + [vmem] * group, [(hbm, query_rows.shape, bf16)] * 2,
            2 * heads * group, member_arg, *pieces,
        )

    layer_out, query_grad = unpacked(first_out, 1, heads)
    key_grad, value_grad = unpacked(last_out, 2, 1)
    return (
        layer_out,
        query_grad,
        key_grad,
        value_grad,
        table_grad.transpose(1, 0, 2),
        sums[:, 1],
    )


def fits_groups(heads_here, rows, seq_count):
    group = WINDOW // rows
    levels_fit = (WINDOW // BLOCK).bit_length() + 1 == LEVELS
    return (
        group * rows == WINDOW
        and rows == 2 * 128
        and group == 1 << (group.bit_length() - 1)
        and heads_here % group == 0
        and seq_count % group == 0
        and seq_count == 1 << (seq_count.bit_length() - 1)
        and levels_fit
    )


def shards(query_rows, *others):
    heads_here, rows, _ = query_rows.shape
    if fits_groups(heads_here, rows, lax.axis_size("seq")):
        return grouped_shards(query_rows, *others)
    return wide_shards(query_rows, *others)


def solution(mesh):
    placed = (
        P("head", "seq", None),
        P("head", "seq", None),
        P("head", "seq", None),
        P("head", None),
        P(None, "head", None),
        P("seq", None),
        P("head"),
        P("head", "seq", None),
    )
    return jax.shard_map(
        shards,
        mesh=mesh,
        in_specs=placed,
        out_specs=(
            P("head", "seq", None),
            P("head", "seq", None),
            P("head", "seq", None),
            P("head", "seq", None),
            P(None, "head", None),
            P("head", None),
        ),
        check_vma=False,
    )
```

```python
import functools
import math

import jax
import jax.numpy as jnp
from jax import lax
from jax.experimental import pallas as pl
from jax.experimental.pallas import tpu as pltpu
from jax.sharding import PartitionSpec as P


H = 16
BLOCK = 64
WINDOW = 1024
LEVELS = 6
TABLE_ROWS = 16


epsilon = 1e-06
block_cap = 512


def shifted(block, axis, distance):
    devices = range(lax.axis_size(axis))
    route = [(i - distance, i) for i in devices if i - distance in devices]
    return lax.ppermute(block, axis, route)


def from_partner(shard, axis, bit):
    return lax.ppermute(shard, axis, [(i, i ^ 1 << bit) for i in range(lax.axis_size(axis))])


def contract(pattern, left_side, right_side):
    return jnp.einsum(pattern, left_side, right_side, preferred_element_type=jnp.float32)


def causal_mask():
    row_pos = lax.broadcasted_iota(jnp.int32, (BLOCK, BLOCK), 0)
    col_pos = lax.broadcasted_iota(jnp.int32, (BLOCK, BLOCK), 1)
    return row_pos >= col_pos


def window_mask(block_rows, shift_rows, key_count, span_len):
    query_pos = lax.broadcasted_iota(jnp.int32, (block_rows, key_count), 0)
    key_pos = lax.broadcasted_iota(jnp.int32, (block_rows, key_count), 1)
    offset = query_pos + shift_rows - key_pos
    return (offset >= 0) & (offset < span_len)


def leaf_view(tensor):
    head_count, token_count, head_dim = tensor.shape
    return tensor.reshape(head_count, token_count // BLOCK, BLOCK, head_dim)


def split_level(tensor, group_len):
    head_count, token_count, head_dim = tensor.shape
    return tensor.reshape(head_count, token_count // (2 * group_len), 2, group_len, head_dim)


def level_summary(key_rows, value_rows, group_len):
    lower_sum = contract(
        "hpse,hpsf->hpef",
        split_level(key_rows, group_len)[:, :, 0],
        split_level(value_rows, group_len)[:, :, 0],
    )
    return (lower_sum * (1.0 / math.sqrt(group_len * key_rows.shape[-1]))).astype(jnp.bfloat16)


def level_area(query_rows, summary, group_len):
    upper_half = contract("hpse,hpef->hpsf", split_level(query_rows, group_len)[:, :, 1], summary)
    return jnp.stack([jnp.zeros_like(upper_half), upper_half], axis=2).reshape(query_rows.shape)


def level_grads(query_rows, key_rows, value_rows, summary, upstream, group_len):
    upstream_up = split_level(upstream, group_len)[:, :, 1]
    query_up = contract("hpsf,hpef->hpse", upstream_up, summary)
    summary_grad = contract(
        "hpse,hpsf->hpef", split_level(query_rows, group_len)[:, :, 1], upstream_up
    )
    low_grad = (summary_grad * (1.0 / math.sqrt(group_len * query_rows.shape[-1]))).astype(
        jnp.bfloat16
    )
    key_low = contract("hpsf,hpef->hpse", split_level(value_rows, group_len)[:, :, 0], low_grad)
    value_low = contract("hpse,hpef->hpsf", split_level(key_rows, group_len)[:, :, 0], low_grad)
    blank = jnp.zeros_like(query_up)
    full_shape = query_rows.shape
    return (
        jnp.stack([blank, query_up], axis=2).reshape(full_shape),
        jnp.stack([key_low, blank], axis=2).reshape(full_shape),
        jnp.stack([value_low, blank], axis=2).reshape(full_shape),
    )


def window_head(query_head, key_head, value_head, span_len):
    token_count, head_dim = query_head.shape
    block_rows = min(block_cap, token_count)
    score_scale = lax.rsqrt((head_dim * span_len).astype(jnp.float32))
    inside = window_mask(block_rows, WINDOW, WINDOW + block_rows, span_len)
    scores = contract("qe,ke->qk", query_head, key_head) * score_scale
    prob_low = jnp.where(inside, scores, 0.0).astype(jnp.bfloat16)
    outputs = [contract("qk,ke->qe", prob_low, value_head)]
    return jnp.concatenate(outputs, axis=0)


def window_back_head(query_head, key_head, value_head, grad_head, span_len, keep_from):
    token_count, head_dim = query_head.shape
    block_rows = min(block_cap, token_count)
    score_scale = lax.rsqrt((head_dim * span_len).astype(jnp.float32))
    inside = window_mask(block_rows, WINDOW, WINDOW + block_rows, span_len)
    key_grad = jnp.zeros((WINDOW + token_count - keep_from, head_dim), jnp.float32)
    value_grad = jnp.zeros((WINDOW + token_count - keep_from, head_dim), jnp.float32)
    grad_part = grad_head[0:block_rows]
    scores = contract("qe,ke->qk", query_head, key_head) * score_scale
    prob_low = jnp.where(inside, scores, 0.0).astype(jnp.bfloat16)
    prob_grad = contract("qe,ke->qk", grad_part, value_head)
    score_grad = jnp.where(inside, prob_grad * score_scale, 0.0).astype(jnp.bfloat16)
    query_grad = [contract("qk,ke->qe", score_grad, key_head)]
    skip_cols = max(keep_from, 0)
    target = skip_cols - keep_from
    length_now = WINDOW + block_rows - skip_cols
    key_grad = key_grad.at[target : target + length_now].add(
        contract("qk,qe->ke", score_grad[:, skip_cols:], query_head)
    )
    value_grad = value_grad.at[target : target + length_now].add(
        contract("qk,qe->ke", prob_low, grad_part)
    )
    return (jnp.concatenate(query_grad, axis=0), key_grad, value_grad)


def wide_shards(
    query_rows, key_rows, value_rows, norm_gain, level_table, level_index, window_length, out_grad
):
    heads_here, tok_here, head_dim = query_rows.shape
    seq_index = lax.axis_index("seq")
    seq_levels = lax.axis_size("seq").bit_length() - 1
    local_levels = (tok_here // BLOCK).bit_length() - 1
    reach_count = WINDOW // tok_here
    onehot = (
        level_index[:, :, None] == lax.broadcasted_iota(jnp.int32, (1, 1, TABLE_ROWS), 2)
    ).astype(jnp.float32)
    weights = jnp.einsum("tjk,khj->htj", onehot, level_table, precision=lax.Precision.HIGHEST)

    def weight_of(level_no):
        return weights[:, :, min(level_no, LEVELS - 1)][:, :, None]

    own_pair = jnp.stack([key_rows, value_rows])
    pieces = []
    for step_no in range(reach_count, 0, -1):
        pieces.append(shifted(own_pair, "seq", step_no))
    pieces.append(own_pair)
    wide_pair = jnp.concatenate(pieces, axis=2)
    device_summary = contract("hte,htf->hef", key_rows, value_rows)
    sibling = []
    running = device_summary
    for bit_no in range(seq_levels):
        partner = from_partner(running, "seq", bit_no)
        upper_half = seq_index >> bit_no & 1 == 1
        sibling.append(jnp.where(upper_half, partner, 0.0))
        running = running + partner
    query_leaf = leaf_view(query_rows)
    key_leaf = leaf_view(key_rows)
    value_leaf = leaf_view(value_rows)
    leaf_scale = 1.0 / math.sqrt(BLOCK * head_dim)
    causal = causal_mask()
    leaf_prob = jnp.where(
        causal, contract("hcte,hcse->hcts", query_leaf, key_leaf) * leaf_scale, 0.0
    ).astype(jnp.bfloat16)
    area_list = [contract("hcts,hcse->hcte", leaf_prob, value_leaf).reshape(query_rows.shape)]
    summaries = []
    for level_no in range(1, local_levels + 1):
        group_len = BLOCK * 2 ** (level_no - 1)
        summary = level_summary(key_rows, value_rows, group_len)
        summaries.append(summary)
        area_list.append(level_area(query_rows, summary, group_len))
    for bit_no in range(seq_levels):
        group_len = tok_here * 2**bit_no
        summary = (sibling[bit_no] * (1.0 / math.sqrt(group_len * head_dim))).astype(jnp.bfloat16)
        summaries.append(summary)
        area_list.append(contract("hte,hef->htf", query_rows, summary))
    mixed = lax.map(
        lambda head_items: window_head(head_items[0], head_items[1], head_items[2], head_items[3]),
        (query_rows, wide_pair[0], wide_pair[1], window_length),
    )
    for level_no in range(len(area_list)):
        mixed = mixed + weight_of(level_no) * area_list[level_no]
    grad_full = out_grad.astype(jnp.float32)
    scaled = grad_full * norm_gain[:, None, :]
    square_sum, cross_sum = lax.psum(
        (jnp.sum(mixed * mixed, axis=(0, 2)), jnp.sum(scaled * mixed, axis=(0, 2))), "head"
    )
    inv_rms = lax.rsqrt(square_sum / (H * head_dim) + epsilon)
    layer_out = (mixed * inv_rms[None, :, None] * norm_gain[:, None, :]).astype(jnp.bfloat16)
    mixed_grad = (
        scaled * inv_rms[None, :, None]
        - mixed * (inv_rms**3 * cross_sum / (H * head_dim))[None, :, None]
    )
    gain_part = jnp.sum(grad_full * mixed * inv_rms[None, :, None], axis=1)
    grad_low = mixed_grad.astype(jnp.bfloat16)
    columns = [jnp.zeros((heads_here, tok_here), jnp.float32) for _ in range(LEVELS)]
    for level_no in range(len(area_list)):
        column_no = min(level_no, LEVELS - 1)
        columns[column_no] = columns[column_no] + jnp.sum(mixed_grad * area_list[level_no], axis=2)
    upstream_leaf = leaf_view((weight_of(0) * mixed_grad).astype(jnp.bfloat16))
    prob_grad = contract("hcte,hcse->hcts", upstream_leaf, value_leaf)
    score_grad = jnp.where(causal, prob_grad * leaf_scale, 0.0).astype(jnp.bfloat16)
    query_grad = contract("hcts,hcse->hcte", score_grad, key_leaf).reshape(query_rows.shape)
    key_grad = contract("hcts,hcte->hcse", score_grad, query_leaf).reshape(query_rows.shape)
    value_grad = contract("hcts,hcte->hcse", leaf_prob, upstream_leaf).reshape(query_rows.shape)
    for level_no in range(1, local_levels + 1):
        group_len = BLOCK * 2 ** (level_no - 1)
        upstream = (weight_of(level_no) * mixed_grad).astype(jnp.bfloat16)
        query_part, key_part, value_part = level_grads(
            query_rows, key_rows, value_rows, summaries[level_no - 1], upstream, group_len
        )
        query_grad = query_grad + query_part
        key_grad = key_grad + key_part
        value_grad = value_grad + value_part
    summary_grads = []
    for bit_no in range(seq_levels):
        level_no = local_levels + 1 + bit_no
        upstream = (weight_of(level_no) * mixed_grad).astype(jnp.bfloat16)
        query_grad = query_grad + contract("htf,hef->hte", upstream, summaries[level_no - 1])
        group_len = tok_here * 2**bit_no
        partial_value = contract("hte,htf->hef", query_rows, upstream) * (
            1.0 / math.sqrt(group_len * head_dim)
        )
        upper_half = seq_index >> bit_no & 1 == 1
        summary_grads.append(jnp.where(upper_half, partial_value, 0.0))
    pending = jnp.stack(summary_grads)
    for bit_no in range(seq_levels):
        partner = from_partner(pending[bit_no:], "seq", bit_no)
        lower_half = seq_index >> bit_no & 1 == 0
        received = jnp.where(lower_half, partner[0], 0.0).astype(jnp.bfloat16)
        key_grad = key_grad + contract("htf,hef->hte", value_rows, received)
        value_grad = value_grad + contract("hte,hef->htf", key_rows, received)
        pending = jnp.concatenate(
            [pending[: bit_no + 1], pending[bit_no + 1 :] + partner[1:]], axis=0
        )
    keep_from = 0
    window_query, window_key, window_value = lax.map(
        lambda head_items: window_back_head(
            head_items[0], head_items[1], head_items[2], head_items[3], head_items[4], keep_from
        ),
        (query_rows, wide_pair[0], wide_pair[1], grad_low, window_length),
    )
    query_grad = query_grad + window_query
    key_grad = key_grad + window_key[:, WINDOW:]
    value_grad = value_grad + window_value[:, WINDOW:]
    for step_no in range(1, reach_count + 1):
        first_row = (reach_count - step_no) * tok_here
        piece = jnp.stack(
            [
                window_key[:, first_row : first_row + tok_here],
                window_value[:, first_row : first_row + tok_here],
            ]
        )
        arrived = shifted(piece.astype(jnp.bfloat16), "seq", -step_no).astype(piece.dtype)
        key_grad = key_grad + arrived[0]
        value_grad = value_grad + arrived[1]
    weight_grad = jnp.stack(columns, axis=-1)
    table_part = jnp.einsum("tjk,htj->khj", onehot, weight_grad, precision=lax.Precision.HIGHEST)
    table_grad, gain_grad = lax.psum((table_part, gain_part), "seq")
    return (
        layer_out,
        query_grad.astype(jnp.bfloat16),
        key_grad.astype(jnp.bfloat16),
        value_grad.astype(jnp.bfloat16),
        table_grad,
        gain_grad,
    )


f32 = jnp.float32
bf16 = jnp.bfloat16
index_rows = 16
kernel_vmem = 16 * 2**20


def dot_nn(left, right):
    return lax.dot_general(left, right, (((1,), (0,)), ((), ())), preferred_element_type=f32)


def dot_nt(left, right):
    return lax.dot_general(left, right, (((1,), (1,)), ((), ())), preferred_element_type=f32)


def dot_tn(left, right):
    return lax.dot_general(left, right, (((0,), (0,)), ((), ())), preferred_element_type=f32)


def added(parts):
    return functools.reduce(lambda a, b: a + b, parts)


def level_scale(level_no, head_dim):
    return 1.0 / math.sqrt(BLOCK * 2 ** max(level_no - 1, 0) * head_dim)


def lane_indices(index_block):
    rows = index_block.astype(f32)
    return jnp.concatenate([rows[:8], rows[8:]], axis=1)


def lane_weights(indices, table_ref):
    weights = jnp.zeros(indices.shape, f32)
    wide = indices.shape[1] // table_ref.shape[-1]
    for row_no in range(TABLE_ROWS):
        row = jnp.concatenate([table_ref[0, row_no]] * wide, axis=1)
        weights = jnp.where(indices == row_no, row, weights)
    return weights


def positions(rows, cols):
    row_pos = lax.broadcasted_iota(jnp.int32, (rows, cols), 0)
    col_pos = lax.broadcasted_iota(jnp.int32, (rows, cols), 1)
    return row_pos, col_pos


def diagonal_factor(query_pos, key_pos, picked, window_scale, near_levels, head_dim):
    shift = BLOCK.bit_length() - 1
    apart = (query_pos >> shift) ^ (key_pos >> shift)
    factor = picked(0) * level_scale(0, head_dim) + window_scale
    for level_no in range(1, near_levels + 1):
        factor = jnp.where(
            apart >= 2 ** (level_no - 1),
            picked(level_no) * level_scale(level_no, head_dim) + window_scale,
            factor,
        )
    return jnp.where(query_pos >= key_pos, factor, 0.0)


def place(target, first_block, piece_refs, member):
    rows = piece_refs[0].shape[0]
    for bits, piece_ref in enumerate(piece_refs):
        start = pl.multiple_of((first_block + (member ^ bits)) * rows, rows)
        target[pl.ds(start, rows)] = piece_ref[...]


def copy_all(pairs, semaphore):
    copies = [pltpu.make_async_copy(a, b, semaphore.at[i]) for i, (a, b) in enumerate(pairs)]
    for copy in copies:
        copy.start()
    for copy in copies:
        copy.wait()


def pack_kernel(member_ref, *refs, group, extra):
    *refs, semaphore = refs
    sources, pieces = refs[:-group], refs[-group:]
    heads = sources[0].shape[0] // group
    rows = sources[0].shape[1]
    pairs = []
    for bits, piece in enumerate(pieces):
        for source_no, source in enumerate(sources[: len(sources) - extra]):
            for head_no in range(heads):
                first = (source_no * heads + head_no) * rows
                block = source.at[(member_ref[0] ^ bits) * heads + head_no]
                pairs.append((block, piece.at[pl.ds(first, rows)]))
        if extra:
            first = (len(sources) - 1) * heads * rows
            pairs.append((sources[-1], piece.at[pl.ds(first, sources[-1].shape[0])]))
    copy_all(pairs, semaphore)


def arrange_kernel(member_ref, *refs, group):
    pieces, (query_ref, grad_ref) = refs[:group], refs[group:]
    count = grad_ref.shape[1]
    for bits, piece in enumerate(pieces):
        block_no = member_ref[0] ^ bits
        query_ref[block_no, :count] = piece[:count]
        query_ref[block_no, count:] = piece[2 * count :]
        grad_ref[block_no] = piece[count : 2 * count]


def unpack_kernel(member_ref, *refs, group, head_stride, kind_stride):
    *refs, semaphore = refs
    pieces, outs = refs[:group], refs[group:]
    heads = outs[0].shape[0] // group
    rows = outs[0].shape[1]
    pairs = []
    for bits, piece in enumerate(pieces):
        for head_no in range(heads):
            for kind, out in enumerate(outs):
                first = (head_no * head_stride + kind * kind_stride) * rows
                target = out.at[(member_ref[0] ^ bits) * heads + head_no]
                pairs.append((piece.at[pl.ds(first, rows)], target))
    copy_all(pairs, semaphore)


def window_reach(span, rows):
    whole = span // rows
    return whole, span - whole * rows


def window_state(blocks, whole, steps):
    state = blocks[0]
    for step_no in range(1, steps):
        state = state + blocks[step_no] * jnp.where(whole > step_no + 1, 1.0, 0.0)
    return state


def summary_kernel(member_ref, *refs, group, near_levels):
    key_refs, value_refs = refs[:group], refs[group : 2 * group]
    near_ref, block_ref, total_ref = refs[2 * group : 2 * group + 3]
    key_all, value_all = refs[2 * group + 3 :]
    rows, head_dim = key_refs[0].shape
    member = member_ref[0]
    place(key_all, 0, key_refs, member)
    place(value_all, 0, value_refs, member)
    parts = [
        dot_tn(key_all[i * rows : (i + 1) * rows], value_all[i * rows : (i + 1) * rows])
        for i in range(group)
    ]
    total_ref[0] = added(parts).astype(bf16)
    for block_no in range(group):
        block_ref[0, block_no] = parts[block_no]
        for bit_no in range(group.bit_length() - 1):
            if block_no >> bit_no & 1:
                first = (block_no >> bit_no << bit_no) - 2**bit_no
                scale = level_scale(near_levels + 1 + bit_no, head_dim)
                lower = added(parts[first : first + 2**bit_no]) * scale
                near_ref[0, block_no, bit_no] = lower.astype(bf16)
            else:
                near_ref[0, block_no, bit_no] = jnp.zeros((head_dim, head_dim), bf16)


def load_window(member, own_refs, prev_refs, target):
    group = len(own_refs)
    rows, head_dim = own_refs[0].shape
    target[:rows] = jnp.zeros((rows, head_dim), bf16)
    place(target, 1, prev_refs, member)
    place(target, 1 + group, own_refs, member)


def forward_kernel(
    member_ref, length_ref, scale_ref, far_scale_ref, *refs, group, chunks, near_levels
):
    key_refs, value_refs = refs[:group], refs[group : 2 * group]
    key_prev, value_prev = refs[2 * group : 3 * group], refs[3 * group : 4 * group]
    (
        query_ref, grad_ref, index_ref, table_ref, gain_ref, near_ref, block_ref,
    ) = refs[4 * group : 4 * group + 7]
    far_refs = refs[4 * group + 7 : 4 * group + chunks + 5]
    (
        mixed_ref, stat_ref, state_ref, far_out_ref, key_all, value_all,
    ) = refs[4 * group + chunks + 5 :]
    head_no = pl.program_id(0)
    _, rows, head_dim = query_ref.shape
    member = member_ref[0]
    load_window(member, key_refs, key_prev, key_all)
    load_window(member, value_refs, value_prev, value_all)
    whole, part = window_reach(length_ref[head_no], rows)
    window_scale = scale_ref[head_no]
    blocks = [
        dot_tn(key_all[i * rows : (i + 1) * rows], value_all[i * rows : (i + 1) * rows])
        for i in range(1, group + 1)
    ]
    far = added(blocks) * far_scale_ref[0]
    for step_no, far_ref in enumerate(far_refs):
        far = far + far_ref[0].astype(f32) * far_scale_ref[step_no + 1]
    far = far.astype(bf16)
    far_out_ref[0] = far
    blocks = blocks[1:] + [block_ref[0, i] for i in range(group - 1)]
    stat_rows = []
    row_pos, col_pos = positions(rows, rows)
    edge_row, edge_col = positions(rows, 2 * rows)
    edge_mask = edge_row - edge_col < part - rows
    ones = jnp.ones((8, head_dim), bf16)
    for block_no in range(group):
        query = query_ref[block_no]
        start = pl.multiple_of((block_no + group - whole) * rows, rows)
        scores = dot_nt(query, key_all[pl.ds(start, 2 * rows)])
        edge = jnp.where(edge_mask, scores, 0.0).astype(bf16)
        total = dot_nn(edge, value_all[pl.ds(start, 2 * rows)])
        recent = blocks[block_no : block_no + group - 1][::-1]
        state = window_state(recent, whole, group - 1) * window_scale
        state = state.astype(bf16)
        state_ref[0, block_no] = state
        weights = jnp.transpose(lane_weights(lane_indices(index_ref[block_no]), table_ref))

        def picked(level_no):
            return weights[:, level_no : level_no + 1]

        factor = diagonal_factor(row_pos, col_pos, picked, window_scale, near_levels, head_dim)
        own = slice((1 + group + block_no) * rows, (2 + group + block_no) * rows)
        prob = (dot_nt(query, key_all[own]) * factor).astype(bf16)
        mixed = dot_nn(prob, value_all[own]) + window_scale * total + dot_nn(query, state)
        for bit_no in range(group.bit_length() - 1):
            if block_no >> bit_no & 1:
                area = dot_nn(query, near_ref[0, block_no, bit_no])
                mixed = mixed + picked(near_levels + 1 + bit_no) * area
        mixed = mixed + picked(LEVELS - 1) * dot_nn(query, far)
        mixed_ref[block_no] = mixed
        scaled = grad_ref[block_no].astype(f32) * gain_ref[0]
        stat_rows.append(dot_nt(ones, (mixed * mixed).astype(bf16))[:1])
        stat_rows.append(dot_nt(ones, (scaled * mixed).astype(bf16))[:1])
    stats = jnp.concatenate(stat_rows, axis=0)

    @pl.when(head_no == 0)
    def _():
        stat_ref[...] = stats

    @pl.when(head_no > 0)
    def _():
        stat_ref[...] = stat_ref[...] + stats


def norm_kernel(member_ref, mixed_ref, grad_ref, gain_ref, *refs, group, width):
    stat_refs, out_refs = refs[:2], refs[2 : 2 + group]
    low_ref, gain_part_ref, out_all = refs[2 + group :]
    gain = gain_ref[0]
    stats = jnp.transpose(added([stat_ref[...] for stat_ref in stat_refs]))
    parts = []
    for block_no in range(group):
        inv_rms = lax.rsqrt(stats[:, 2 * block_no : 2 * block_no + 1] / width + epsilon)
        pull = inv_rms * inv_rms * inv_rms * stats[:, 2 * block_no + 1 : 2 * block_no + 2] / width
        mixed = mixed_ref[block_no]
        grad = grad_ref[block_no].astype(f32)
        normed = mixed * inv_rms
        out_all[block_no] = (normed * gain).astype(bf16)
        low_ref[block_no] = (grad * gain * inv_rms - mixed * pull).astype(bf16)
        parts.append(jnp.sum(grad * normed, axis=0, keepdims=True))
    gain_part_ref[0] = added(parts)
    for bits, out_ref in enumerate(out_refs):
        out_ref[...] = out_all[member_ref[0] ^ bits]


def last_level_outer(query_ref, low_ref, index_ref, table_ref):
    parts = []
    for block_no in range(query_ref.shape[0]):
        weights = jnp.transpose(lane_weights(lane_indices(index_ref[block_no]), table_ref))
        low = weights[:, LEVELS - 1 : LEVELS] * low_ref[block_no].astype(f32)
        parts.append(dot_tn(query_ref[block_no], low.astype(bf16)))
    return added(parts)


def far_grad_kernel(query_ref, low_ref, index_ref, table_ref, far_grad_ref):
    outer = last_level_outer(query_ref, low_ref, index_ref, table_ref)
    far_grad_ref[0] = outer.astype(bf16)


def query_kernel(member_ref, length_ref, scale_ref, *refs, group, near_levels):
    key_refs, value_refs = refs[:group], refs[group : 2 * group]
    key_prev, value_prev = refs[2 * group : 3 * group], refs[3 * group : 4 * group]
    (
        query_ref, low_ref, index_ref, table_ref, near_ref, state_ref, far_ref, gain_part_ref,
    ) = refs[4 * group : 4 * group + 8]
    out_refs = refs[5 * group + 8 : 6 * group + 8]
    near_grad_ref, sums_ref, key_all, value_all, out_all = refs[6 * group + 8 :]
    head_no = pl.program_id(0)
    _, rows, head_dim = query_ref.shape
    member = member_ref[0]
    load_window(member, key_refs, key_prev, key_all)
    load_window(member, value_refs, value_prev, value_all)
    whole, part = window_reach(length_ref[head_no], rows)
    window_scale = scale_ref[head_no]
    row_pos, col_pos = positions(rows, rows)
    edge_row, edge_col = positions(rows, 2 * rows)
    edge_mask = edge_row - edge_col < part - rows
    ones = jnp.ones((8, head_dim), bf16)
    leaf_row = lax.broadcasted_iota(jnp.int32, (8, rows), 0)
    leaf_col = lax.broadcasted_iota(jnp.int32, (8, rows), 1) >> (BLOCK.bit_length() - 1)
    leaf_pick = jnp.where(leaf_row == leaf_col, 1.0, 0.0).astype(bf16)
    own_leaf = leaf_col[:1]
    lanes = table_ref.shape[-1]
    table_parts = [jnp.zeros((8, lanes), f32) for _ in range(TABLE_ROWS)]
    near_grads = [[] for _ in range(group)]
    for block_no in range(group):
        query = query_ref[block_no]
        low = low_ref[block_no]
        start = pl.multiple_of((block_no + group - whole) * rows, rows)
        scores = dot_nt(low, value_all[pl.ds(start, 2 * rows)])
        edge = jnp.where(edge_mask, scores, 0.0).astype(bf16)
        total = dot_nn(edge, key_all[pl.ds(start, 2 * rows)])
        indices = lane_indices(index_ref[block_no])
        weights = jnp.transpose(lane_weights(indices, table_ref))

        def picked(level_no):
            return weights[:, level_no : level_no + 1]

        factor = diagonal_factor(row_pos, col_pos, picked, window_scale, near_levels, head_dim)
        own = slice((1 + group + block_no) * rows, (2 + group + block_no) * rows)
        prob_grad = dot_nt(low, value_all[own])
        result = dot_nn((prob_grad * factor).astype(bf16), key_all[own])
        result = result + window_scale * total + dot_nt(low, state_ref[0, block_no])
        scores = dot_nt(query, key_all[own])
        pairs = jnp.where(row_pos >= col_pos, scores * prob_grad, 0.0).astype(bf16)
        leaf_sums = dot_nt(leaf_pick, pairs)
        level_rows = [jnp.zeros((1, rows), f32) for _ in range(8)]
        for leaf_no in range(rows // BLOCK):
            leaf_sum = leaf_sums[leaf_no : leaf_no + 1]
            apart = own_leaf ^ leaf_no
            level_rows[0] = level_rows[0] + jnp.where(apart == 0, leaf_sum, 0.0)
            for level_no in range(1, near_levels + 1):
                here = (apart >> (level_no - 1)) == 1
                level_rows[level_no] = level_rows[level_no] + jnp.where(here, leaf_sum, 0.0)
        for level_no in range(near_levels + 1):
            level_rows[level_no] = level_rows[level_no] * level_scale(level_no, head_dim)
        query_wide = query.astype(f32)
        low_wide = low.astype(f32)
        for level_no in range(near_levels + 1, LEVELS):
            bit_no = level_no - near_levels - 1
            last = level_no == LEVELS - 1
            if not last and not block_no >> bit_no & 1:
                continue
            back = dot_nt(low, far_ref[0] if last else near_ref[0, block_no, bit_no])
            result = result + picked(level_no) * back
            level_rows[level_no] = dot_nt(ones, (query_wide * back).astype(bf16))[:1]
            if not last:
                upstream = (picked(level_no) * low_wide).astype(bf16)
                outer = dot_tn(query, upstream) * level_scale(level_no, head_dim)
                first = ((block_no >> bit_no) - 1) << bit_no
                for lower_no in range(first, first + 2**bit_no):
                    near_grads[lower_no].append(outer)
        out_all[block_no] = result.astype(bf16)
        weight_grad = jnp.concatenate(level_rows, axis=0)
        for row_no in range(TABLE_ROWS):
            chosen = jnp.where(indices == row_no, weight_grad, 0.0)
            folded = added([chosen[:, i : i + lanes] for i in range(0, rows, lanes)])
            table_parts[row_no] = table_parts[row_no] + folded
    table_part = jnp.concatenate(table_parts, axis=0)
    table_high = table_part.astype(bf16)
    table_low = (table_part - table_high.astype(f32)).astype(bf16)
    lane_sums = dot_nt(ones, table_high) + dot_nt(ones, table_low)
    for bits, out_ref in enumerate(out_refs):
        out_ref[...] = out_all[member ^ bits]
    for lower_no in range(group - 1):
        near_grad_ref[0, lower_no] = added(near_grads[lower_no])
    heads = pl.num_programs(0)
    row_no = lax.broadcasted_iota(jnp.int32, sums_ref.shape, 0)
    first = (member * heads + head_no) * 2

    @pl.when(head_no == 0)
    def _():
        sums_ref[...] = jnp.zeros(sums_ref.shape, f32)

    sums = jnp.where(row_no == first, lane_sums[:1], sums_ref[...])
    sums_ref[...] = jnp.where(row_no == first + 1, gain_part_ref[0], sums)


def key_kernel(
    member_ref, length_ref, scale_ref, far_scale_ref, *refs, group, chunks, near_levels
):
    key_refs, value_refs = refs[:group], refs[group : 2 * group]
    (
        query_ref, low_ref, query_next_ref, low_next_ref, index_ref, index_next_ref, table_ref,
        near_grad_ref,
    ) = refs[2 * group : 2 * group + 8]
    far_refs = refs[2 * group + 8 : 2 * group + chunks + 6]
    out_refs = refs[2 * group + chunks + 6 : 3 * group + chunks + 6]
    key_all, value_all, query_all, low_all, out_all = refs[3 * group + chunks + 6 :]
    head_no = pl.program_id(0)
    _, rows, head_dim = query_ref.shape
    member = member_ref[0]
    place(key_all, 0, key_refs, member)
    place(value_all, 0, value_refs, member)
    for target, first_ref, second_ref in (
        (query_all, query_ref, query_next_ref),
        (low_all, low_ref, low_next_ref),
    ):
        for i in range(group):
            target[i * rows : (i + 1) * rows] = first_ref[i]
            target[(group + i) * rows : (group + i + 1) * rows] = second_ref[i]
        target[2 * group * rows :] = jnp.zeros((rows, head_dim), bf16)
    whole, part = window_reach(length_ref[head_no], rows)
    window_scale = scale_ref[head_no]
    blocks = [
        dot_tn(query_all[i * rows : (i + 1) * rows], low_all[i * rows : (i + 1) * rows])
        for i in range(1, 2 * group - 1)
    ]
    far_grad = last_level_outer(query_next_ref, low_next_ref, index_next_ref, table_ref)
    far_grad = far_grad * far_scale_ref[chunks - 1]
    for step_no, far_ref in enumerate(far_refs):
        far_grad = far_grad + far_ref[0].astype(f32) * far_scale_ref[chunks + step_no]
    row_pos, col_pos = positions(rows, rows)
    edge_row, edge_col = positions(rows, 2 * rows)
    edge_mask = edge_col - edge_row < part
    for block_no in range(group):
        own = slice(block_no * rows, (block_no + 1) * rows)
        key = key_all[own]
        value = value_all[own]
        start = pl.multiple_of((block_no + whole) * rows, rows)
        query_part = query_all[pl.ds(start, 2 * rows)]
        low_part = low_all[pl.ds(start, 2 * rows)]
        prob = jnp.where(edge_mask, dot_nt(key, query_part), 0.0).astype(bf16)
        prob_grad = jnp.where(edge_mask, dot_nt(value, low_part), 0.0).astype(bf16)
        value_total = dot_nn(prob, low_part)
        key_total = dot_nn(prob_grad, query_part)
        weights = lane_weights(lane_indices(index_ref[block_no]), table_ref)

        def picked(level_no):
            return weights[level_no : level_no + 1]

        factor = diagonal_factor(col_pos, row_pos, picked, window_scale, near_levels, head_dim)
        prob = (dot_nt(key, query_all[own]) * factor).astype(bf16)
        prob_grad = (dot_nt(value, low_all[own]) * factor).astype(bf16)
        state = window_state(blocks[block_no : block_no + group - 1], whole, group - 1)
        state = state * window_scale + far_grad
        if block_no < group - 1:
            state = state + near_grad_ref[0, block_no]
        state = state.astype(bf16)
        value_grad = dot_nn(prob, low_all[own]) + window_scale * value_total + dot_nn(key, state)
        key_grad = dot_nn(prob_grad, query_all[own]) + window_scale * key_total
        key_grad = key_grad + dot_nt(value, state)
        out_all[block_no, :rows] = key_grad.astype(bf16)
        out_all[block_no, rows:] = value_grad.astype(bf16)
    for bits, out_ref in enumerate(out_refs):
        out_ref[...] = out_all[member ^ bits]


def grouped_shards(
    query_rows, key_rows, value_rows, norm_gain, level_table, level_index, window_length, out_grad
):
    heads_here, rows, head_dim = query_rows.shape
    group = WINDOW // rows
    heads = heads_here // group
    group_bits = group.bit_length() - 1
    near_levels = (rows // BLOCK).bit_length() - 1
    seq_count = lax.axis_size("seq")
    chunks = seq_count // group
    chunk_bits = chunks.bit_length() - 1
    seq_index = lax.axis_index("seq")
    member = seq_index & (group - 1)
    member_arg = member.astype(jnp.int32).reshape(1)
    head_count = lax.axis_size("head")
    width = float(heads_here * head_count * head_dim)

    first_head = member * heads
    table = lax.dynamic_slice_in_dim(level_table, first_head, heads, 1)
    table = jnp.pad(table.transpose(1, 0, 2), ((0, 0), (0, 0), (0, 8 - LEVELS)))
    gain = lax.dynamic_slice_in_dim(norm_gain, first_head, heads, 0)[:, None, :]
    length = lax.dynamic_slice_in_dim(window_length, first_head, heads, 0)
    scale = lax.rsqrt((head_dim * length).astype(f32))
    chunk_no = (seq_index >> group_bits).astype(jnp.int32)
    steps = lax.broadcasted_iota(jnp.int32, (2 * chunks - 2,), 0)
    steps = jnp.where(steps < chunks - 1, -1 - steps, steps - chunks + 2)
    apart = chunk_no ^ (chunk_no + steps)
    far_scale = jnp.full(apart.shape, level_scale(near_levels + group_bits + 1, head_dim), f32)
    for bit_no in range(1, chunk_bits):
        scale_here = level_scale(near_levels + group_bits + 1 + bit_no, head_dim)
        far_scale = jnp.where(apart >= 1 << bit_no, scale_here, far_scale)
    early_member = member_arg
    member_arg, length, scale, far_scale, gain, table = lax.optimization_barrier(
        (member_arg, length, scale, far_scale, gain, table)
    )
    table = jnp.broadcast_to(table[..., None], (heads, TABLE_ROWS, 8, 128))

    def swapped(shard, bits):
        return lax.ppermute(shard, "seq", [(i, i ^ bits) for i in range(seq_count)])

    def moved(shard, distance):
        return shifted(shard, "seq", distance)

    def exchanged(pieces):
        return list(pieces[:1]) + [swapped(pieces[bits], bits) for bits in range(1, group)]

    smem = pl.BlockSpec(memory_space=pltpu.SMEM)
    vmem = pl.BlockSpec(memory_space=pltpu.VMEM)
    hbm = pl.BlockSpec(memory_space=pltpu.HBM)

    def whole_call(kernel, in_specs, outs, copies, *args):
        return pl.pallas_call(
            kernel,
            in_specs=in_specs,
            out_specs=[spec for spec, _, _ in outs],
            out_shape=[jax.ShapeDtypeStruct(shape, dtype) for _, shape, dtype in outs],
            scratch_shapes=[pltpu.SemaphoreType.DMA((copies,))] if copies else [],
            compiler_params=pltpu.CompilerParams(vmem_limit_bytes=kernel_vmem),
        )(*args)

    def in_hbm(tensor):
        return pltpu.with_memory_space_constraint(tensor, pltpu.HBM)

    piece_shape = (2 * heads * rows, head_dim)
    rest_shape = (2 * heads * rows + index_rows, head_dim)
    chunk_shape = (group, heads * rows, head_dim)
    query_shape = (group, heads * rows + index_rows, head_dim)
    pair = whole_call(
        functools.partial(pack_kernel, group=group, extra=0),
        [smem, hbm, hbm], [(vmem, piece_shape, bf16)] * group, 2 * heads * group,
        early_member, in_hbm(key_rows), in_hbm(value_rows),
    )
    index_pad = jnp.pad(level_index.astype(bf16), ((0, 0), (0, 8 - LEVELS)))
    index_pack = index_pad.reshape(rows // 128, 128, 8).transpose(0, 2, 1).reshape(index_rows, 128)
    rest = whole_call(
        functools.partial(pack_kernel, group=group, extra=1),
        [smem, hbm, hbm, hbm], [(vmem, rest_shape, bf16)] * group, (2 * heads + 1) * group,
        member_arg, query_rows, out_grad, index_pack,
    )
    pair = exchanged(pair)
    pair_prev = [moved(piece, group) for piece in pair]
    rest = exchanged(rest)
    query, grad = whole_call(
        functools.partial(arrange_kernel, group=group), [smem] + [vmem] * group,
        [(vmem, query_shape, bf16), (vmem, chunk_shape, bf16)], 0,
        member_arg, *rest,
    )
    query_next = moved(query, -group)

    state_shape = (head_dim, head_dim)
    states_shape = (heads,) + state_shape
    near_shape = (heads, group, group_bits) + state_shape
    block_states = (heads, group) + state_shape
    lower_shape = (heads, group - 1) + state_shape

    def whole(first):
        return pl.BlockSpec((group, rows, head_dim), lambda h: (0, first * heads + h, 0))

    def each(first):
        return [pl.BlockSpec((rows, head_dim), lambda h: (first * heads + h, 0))] * group

    def per_head(shape):
        return pl.BlockSpec((1,) + shape[1:], lambda h: (h,) + (0,) * (len(shape) - 1))

    def fixed(shape):
        return pl.BlockSpec(shape, lambda h: (0,) * len(shape))

    index_spec = pl.BlockSpec(
        (group, index_rows, head_dim), lambda h: (0, heads * rows // index_rows, 0)
    )
    table_spec = per_head(table.shape)
    stat_shape = (2 * group, rows)

    def run(kernel, cost, in_specs, outs, scratch, aliases, *args):
        return pl.pallas_call(
            kernel,
            grid=(heads,),
            in_specs=in_specs,
            out_specs=[spec for spec, _, _ in outs],
            out_shape=[jax.ShapeDtypeStruct(shape, dtype) for _, shape, dtype in outs],
            scratch_shapes=[pltpu.VMEM(shape, bf16) for shape in scratch],
            input_output_aliases=aliases,
            cost_estimate=pl.CostEstimate(
                flops=int(cost * 1e9), transcendentals=0, bytes_accessed=4 * 2**20
            ),
            compiler_params=pltpu.CompilerParams(vmem_limit_bytes=kernel_vmem),
        )(*args)

    sizes = dict(group=group, near_levels=near_levels)
    chunk_rows = (group * rows, head_dim)
    window_rows = ((2 * group + 1) * rows, head_dim)
    results = (group, rows, head_dim)
    near, block_sums, total = run(
        functools.partial(summary_kernel, **sizes), 0.5,
        [smem] + each(0) + each(1),
        [
            (per_head(near_shape), near_shape, bf16),
            (per_head(block_states), block_states, f32),
            (per_head(states_shape), states_shape, bf16),
        ],
        [chunk_rows] * 2, {}, member_arg, *pair, *pair,
    )
    far = [moved(total, step_no * group) for step_no in range(2, chunks)]
    far_spec = per_head(states_shape)

    mixed, stats, states, far = run(
        functools.partial(forward_kernel, chunks=chunks, **sizes), 3,
        [smem] * 4 + each(0) + each(1) + each(0) + each(1)
        + [
            whole(0), whole(0), index_spec, table_spec, per_head(gain.shape),
            per_head(near_shape), per_head(block_states),
        ]
        + [far_spec] * (chunks - 2),
        [
            (whole(0), chunk_shape, f32),
            (fixed(stat_shape), stat_shape, f32),
            (per_head(block_states), block_states, bf16),
            (far_spec, states_shape, bf16),
        ],
        [window_rows] * 2, {},
        member_arg, length, scale, far_scale, *pair, *pair, *pair_prev, *pair_prev,
        query, grad, query, table, gain, near, block_sums, *far,
    )

    part = stats
    for step_no in range(1, head_count):
        turn = [(i, (i + step_no) % head_count) for i in range(head_count)]
        stats = stats + lax.ppermute(part, "head", turn)
    for bit_no in range(group_bits - 1):
        stats = stats + swapped(stats, 1 << bit_no)
    stat_parts = [stats, swapped(stats, group >> 1)]

    out_pieces = [(each(0)[0], piece_shape, bf16)] * group
    *first_out, low, gain_part = run(
        functools.partial(norm_kernel, group=group, width=width), 0.6,
        [smem, whole(0), whole(0), per_head(gain.shape)] + [fixed(stat_shape)] * 2,
        out_pieces + [(whole(0), chunk_shape, bf16), (per_head(gain.shape), gain.shape, f32)],
        [results], {}, member_arg, mixed, grad, gain, *stat_parts,
    )
    low_next = moved(low, -group)
    (far_part,) = run(
        far_grad_kernel, 0.3,
        [whole(0), whole(0), index_spec, table_spec], [(far_spec, states_shape, bf16)],
        [], {}, query, low, query, table,
    )
    far_grad = [moved(far_part, -step_no * group) for step_no in range(2, chunks)]

    args = (
        member_arg, length, scale, *pair, *pair, *pair_prev, *pair_prev,
        query, low, query, table, near, states, far, gain_part, *first_out,
    )
    sums_shape = (2 * heads_here, head_dim)
    *first_out, near_grad, sums = run(
        functools.partial(query_kernel, **sizes), 3,
        [smem] * 3 + each(0) + each(1) + each(0) + each(1)
        + [
            whole(0), whole(0), index_spec, table_spec, per_head(near_shape),
            per_head(block_states), far_spec, per_head(gain.shape),
        ]
        + [pl.BlockSpec(memory_space=pl.ANY)] * group,
        [(each(1)[0], piece_shape, bf16)] * group
        + [(per_head(lower_shape), lower_shape, f32), (fixed(sums_shape), sums_shape, f32)],
        [window_rows] * 2 + [results],
        {len(args) - group + bits: bits for bits in range(group)}, *args,
    )
    first_out = exchanged(first_out)

    pair_out = pl.BlockSpec((2 * rows, head_dim), lambda h: (h, 0))
    last_out = run(
        functools.partial(key_kernel, chunks=chunks, **sizes), 4,
        [smem] * 4 + each(0) + each(1)
        + [
            whole(0), whole(0), whole(0), whole(0), index_spec, index_spec, table_spec,
            per_head(lower_shape),
        ]
        + [far_spec] * (chunks - 2),
        [(pair_out, piece_shape, bf16)] * group,
        [chunk_rows] * 2 + [window_rows] * 2 + [(group, 2 * rows, head_dim)], {},
        member_arg, length, scale, far_scale, *pair, *pair,
        query, low, query_next, low_next, query, query_next, table, near_grad, *far_grad,
    )
    last_out = exchanged(last_out)

    for step_no in range(chunk_bits + group_bits):
        sums = sums + swapped(sums, 1 << step_no)
    sums = sums.reshape(heads_here, 2, head_dim)
    table_grad = sums[:, 0].reshape(heads_here, TABLE_ROWS, 8)[:, :, :LEVELS]

    def unpacked(pieces, head_stride, kind_stride):
        return whole_call(
            functools.partial(
                unpack_kernel, group=group, head_stride=head_stride, kind_stride=kind_stride
            ),
            [smem] + [vmem] * group, [(hbm, query_rows.shape, bf16)] * 2,
            2 * heads * group, member_arg, *pieces,
        )

    layer_out, query_grad = unpacked(first_out, 1, heads)
    key_grad, value_grad = unpacked(last_out, 2, 1)
    return (
        layer_out,
        query_grad,
        key_grad,
        value_grad,
        table_grad.transpose(1, 0, 2),
        sums[:, 1],
    )


def fits_groups(heads_here, rows, seq_count):
    group = WINDOW // rows
    levels_fit = (WINDOW // BLOCK).bit_length() + 1 == LEVELS
    return (
        group * rows == WINDOW
        and rows == 2 * 128
        and group == 1 << (group.bit_length() - 1)
        and heads_here % group == 0
        and seq_count % group == 0
        and seq_count > 2 * group
        and seq_count == 1 << (seq_count.bit_length() - 1)
        and levels_fit
    )


def shards(query_rows, *others):
    heads_here, rows, _ = query_rows.shape
    if fits_groups(heads_here, rows, lax.axis_size("seq")):
        return grouped_shards(query_rows, *others)
    return wide_shards(query_rows, *others)


def solution(mesh):
    placed = (
        P("head", "seq", None),
        P("head", "seq", None),
        P("head", "seq", None),
        P("head", None),
        P(None, "head", None),
        P("seq", None),
        P("head"),
        P("head", "seq", None),
    )
    return jax.shard_map(
        shards,
        mesh=mesh,
        in_specs=placed,
        out_specs=(
            P("head", "seq", None),
            P("head", "seq", None),
            P("head", "seq", None),
            P("head", "seq", None),
            P(None, "head", None),
            P("head", None),
        ),
        check_vma=False,
    )
```
